256 devices in a mesh: dp: 4 (over x_hi, core), mp: 64 (over x_lo, y, z).
Axes of the slice: x: 4 (x_hi: 2, x_lo: 2; x = x_hi * 2 + x_lo), y: 4, z: 8, core: 2. Of those that a mesh axis runs over, the one named last changes fastest.
Arguments:
- source_prompts: bfloat16 [128, 64, 4096], P(None, None, 'mp'), may hold values from -6 to 6
- task_logits: float32 [8, 128], replicated, may hold values from -8 to 260
- task_ids: int32 [256], P('dp'), may hold values from 0 to 7
- key_weight: bfloat16 [4096, 4096], P(None, 'mp'), may hold values from -0.09375 to 0.09375
- value_weight: bfloat16 [4096, 4096], P(None, 'mp'), may hold values from -0.09375 to 0.09375
- queries: bfloat16 [256, 128, 4096], P(('dp', 'mp')), may hold values from -32 to 32
- keys: bfloat16 [256, 128, 4096], P(('dp', 'mp')), may hold values from -16 to 16
- values: bfloat16 [256, 128, 4096], P(('dp', 'mp')), may hold values from -6 to 6
- cotangent: bfloat16 [256, 128, 4096], P(('dp', 'mp')), may hold values from -6 to 6
Outputs:
- attended: bfloat16 [256, 128, 4096], P(('dp', 'mp'))
- source_grad: float32 [128, 64, 4096], P(None, 'dp', 'mp')
- logits_grad: float32 [8, 128], replicated
The draws below stay inside these ranges and needn't reach their ends.
All inputs are finite; a program needn't handle non-finite values.
Results may differ from the reference program's by a relative error of at most 0.011.
Values may be sent and summed in bfloat16 or wider, within the bound.
A program may use at most 128 MiB of HBM per device.

```python
import jax
import jax.numpy as jnp
from jax import lax

D = 4096
HEADS = 32
DH = 128
NSRC = 128
NTASK = 8
PTOK = 64
SEQ = 128
EXAMPLES = 256


def query_key_pair(key):
    paired_key = jax.random.fold_in(key, 11)
    query_seed, key_seed = jax.random.split(paired_key, 2)
    full_shape = (EXAMPLES, SEQ, D)
    query_draw = jax.random.normal(query_seed, full_shape, jnp.float32)
    key_draw = jax.random.normal(key_seed, full_shape, jnp.float32)
    return (jnp.clip(query_draw, -32.0, 32.0), jnp.clip(key_draw, -16.0, 16.0))


def draw_queries(key, part):
    return query_key_pair(key)[0].astype(jnp.bfloat16)


def draw_keys(key, part):
    return query_key_pair(key)[1].astype(jnp.bfloat16)


def draw_task_logits(key, part):
    logit_key = jax.random.fold_in(key, 23)
    base_seed = jax.random.fold_in(logit_key, 0)
    logits = jnp.clip(2.0 * jax.random.normal(base_seed, (NTASK, NSRC), jnp.float32), -8.0, 8.0)
    return logits


def plant(result, own_key, smallest, high):
    place = [jax.random.randint(jax.random.fold_in(own_key, axis), (), 0, length) for axis, length in enumerate(result.shape)]
    main_axis = result.shape.index(max(result.shape))
    beside = place[:main_axis] + [(place[main_axis] + 1) % result.shape[main_axis]] + place[main_axis + 1:]
    return result.at[tuple(place)].set(smallest).at[tuple(beside)].set(high)


def steps_of(rng, extent, cuts, least, largest):
    level, own = 1.0, jax.random.fold_in(rng, 6)
    for dim, blocks in cuts:
        steps = jnp.exp(jax.random.uniform(jax.random.fold_in(own, dim), (blocks,), jnp.float32, least / len(cuts), largest / len(cuts)))
        level = level * jnp.repeat(steps, extent[dim] // blocks).reshape([-1 if axis == dim else 1 for axis in range(len(extent))])
    return level


def centred(own_key, shape, scale, limit, pieces=(), kind=jnp.bfloat16):
    loudness = steps_of(own_key, shape, pieces, -0.22, 0.18) if pieces else 1.0
    drawn = jax.random.normal(own_key, shape, jnp.float32) * scale * loudness
    return jnp.minimum(jnp.maximum(drawn, -limit), limit).astype(kind)


def setup_inputs(seed: int = 0) -> dict:
    streams_of = jax.random.split(jax.random.key(seed), 10)
    return {
        "source_prompts": centred(streams_of[0], (NSRC, PTOK, D), 1.0, 6.0, ((2, 64),)),
        "task_logits": draw_task_logits(jax.random.fold_in(streams_of[9], 71), 0),
        "task_ids": plant(jax.random.randint(streams_of[2], (EXAMPLES,), 0, NTASK), jax.random.fold_in(streams_of[2], 1), 0, NTASK - 1).astype(jnp.int32),
        "key_weight": centred(streams_of[3], (D, D), D ** -0.5, 0.09375, ((1, 64),)),
        "value_weight": centred(streams_of[4], (D, D), D ** -0.5, 0.09375, ((1, 64),)),
        "queries": draw_queries(jax.random.fold_in(streams_of[9], 71), 0),
        "keys": draw_keys(jax.random.fold_in(streams_of[9], 71), 0),
        "values": centred(streams_of[7], (EXAMPLES, SEQ, D), 1.0, 6.0, ((0, 256),)),
        "cotangent": centred(streams_of[8], (EXAMPLES, SEQ, D), 1.0, 6.0, ((0, 256),)),
    }


mask_fill = -1.0e30


def example_pass(prompt_pair, query_rows, key_rows, value_rows, cot_rows):
    score_scale = DH ** -0.5
    key_all = jnp.concatenate([prompt_pair[:, 0, :], key_rows], axis=0)
    value_all = jnp.concatenate([prompt_pair[:, 1, :], value_rows], axis=0)
    query_heads = query_rows.astype(jnp.float32).reshape(SEQ, HEADS, DH)
    key_heads = key_all.astype(jnp.float32).reshape(PTOK + SEQ, HEADS, DH)
    value_heads = value_all.astype(jnp.float32).reshape(PTOK + SEQ, HEADS, DH)
    cot_heads = cot_rows.astype(jnp.float32).reshape(SEQ, HEADS, DH)
    scores = jnp.einsum("ihd,jhd->hij", query_heads, key_heads) * score_scale
    column = jnp.arange(PTOK + SEQ)[None, :]
    position = jnp.arange(SEQ)[:, None]
    visible = (column < PTOK) | (column - PTOK <= position)
    scores = jnp.where(visible[None], scores, mask_fill)
    top_score = jnp.max(scores, axis=2, keepdims=True)
    exponent = jnp.exp(scores - top_score)
    attention = exponent / jnp.sum(exponent, axis=2, keepdims=True)
    attention_rounded = attention.astype(jnp.bfloat16)
    attended = jnp.einsum("hij,jhd->ihd", attention_rounded.astype(jnp.float32), value_heads)
    attended = attended.astype(jnp.bfloat16).reshape(SEQ, D)
    grad_attention = jnp.einsum("ihd,jhd->hij", cot_heads, value_heads)
    inner_sum = jnp.sum(attention * grad_attention, axis=2, keepdims=True)
    grad_scores = (attention * (grad_attention - inner_sum)).astype(jnp.bfloat16)
    key_grads = jnp.einsum("hij,ihd->jhd", grad_scores[:, :, :PTOK].astype(jnp.float32), query_heads)
    key_grads = (key_grads * score_scale).astype(jnp.bfloat16)
    value_grads = jnp.einsum("hij,ihd->jhd", attention_rounded[:, :, :PTOK].astype(jnp.float32), cot_heads)
    value_grads = value_grads.astype(jnp.bfloat16)
    return attended, jnp.stack([key_grads.reshape(PTOK, D), value_grads.reshape(PTOK, D)], axis=1)


def reference(source_prompts, task_logits, task_ids, key_weight, value_weight, queries, keys, values, cotangent):
    mix_weights = jax.nn.softmax(task_logits, axis=1)
    mix_rounded = mix_weights.astype(jnp.bfloat16)
    mixture = jnp.dot(mix_rounded, source_prompts.reshape(NSRC, PTOK * D), preferred_element_type=jnp.float32)
    mixture = mixture.astype(jnp.bfloat16).reshape(NTASK * PTOK, D)
    prompt_keys = jnp.dot(mixture, key_weight, preferred_element_type=jnp.float32).astype(jnp.bfloat16)
    prompt_values = jnp.dot(mixture, value_weight, preferred_element_type=jnp.float32).astype(jnp.bfloat16)
    prompt_table = jnp.stack([prompt_keys, prompt_values], axis=1).reshape(NTASK, PTOK, 2, D)

    def one_example(packed):
        task_index, query_rows, key_rows, value_rows, cot_rows = packed
        prompt_pair = lax.dynamic_index_in_dim(prompt_table, task_index, 0, keepdims=False)
        return example_pass(prompt_pair, query_rows, key_rows, value_rows, cot_rows)

    attended, prompt_grads = lax.map(one_example, (task_ids, queries, keys, values, cotangent))
    selector = (task_ids[:, None] == jnp.arange(NTASK, dtype=jnp.int32)[None, :]).astype(jnp.float32)
    task_grads = jnp.dot(selector.T, prompt_grads.reshape(EXAMPLES, PTOK * 2 * D).astype(jnp.float32),
                         precision=lax.Precision.HIGHEST)
    task_grads = task_grads.reshape(NTASK * PTOK, 2, D)
    mixture_grad = jnp.dot(task_grads[:, 0, :], key_weight.astype(jnp.float32).T, precision=lax.Precision.HIGHEST)
    mixture_grad = mixture_grad + jnp.dot(task_grads[:, 1, :], value_weight.astype(jnp.float32).T,
                                          precision=lax.Precision.HIGHEST)
    mixture_grad = mixture_grad.reshape(NTASK, PTOK * D)
    source_grad = jnp.dot(mix_weights.T, mixture_grad, precision=lax.Precision.HIGHEST).reshape(NSRC, PTOK, D)
    weight_grad = jnp.dot(mixture_grad, source_prompts.reshape(NSRC, PTOK * D).astype(jnp.float32).T,
                          precision=lax.Precision.HIGHEST)
    logits_grad = mix_weights * (weight_grad - jnp.sum(mix_weights * weight_grad, axis=1, keepdims=True))
    return attended, source_grad, logits_grad
```

```python
import functools

import jax
import jax.numpy as jnp
from jax import lax
from jax.experimental import pallas as pl
from jax.experimental.pallas import tpu as pltpu
from jax.sharding import Mesh
from jax.sharding import PartitionSpec as P

D = 4096
HEADS = 32
DH = 128
NSRC = 128
NTASK = 8
PTOK = 64
SEQ = 128
AXES = ("dp_0", "dp_1", "mp_0", "mp_1", "mp_2")
MP = ("mp_0", "mp_1", "mp_2")
DP = ("dp_0", "dp_1")
MESH = pl.DeviceIdType.MESH
ROWS = 16
COLS = 64
PLANE = 32
F32 = jnp.float32
BF16 = jnp.bfloat16
HIGH = lax.Precision.HIGHEST


def here():
    return tuple(lax.axis_index(name) for name in AXES)


def plane_index(a, c, x, y):
    return ((a * 2 + c) * 2 + x) * 4 + y


def plane_device(p):
    return {
        "dp_0": lax.div(p, 16),
        "dp_1": lax.rem(lax.div(p, 8), 2),
        "mp_0": lax.rem(lax.div(p, 4), 2),
        "mp_1": lax.rem(p, 4),
    }


def push(src, dst, sent, landed, device):
    return pltpu.make_async_remote_copy(
        src_ref=src, dst_ref=dst, send_sem=sent, recv_sem=landed, device_id=device, device_id_type=MESH
    )


def greet(me, z):
    barrier = pltpu.get_barrier_semaphore()

    def plane(o, carry):
        pl.semaphore_signal(barrier, inc=1, device_id=plane_device(lax.rem(me + o, PLANE)), device_id_type=MESH)
        return carry

    lax.fori_loop(1, PLANE, plane, 0)
    for o in range(1, 8):
        pl.semaphore_signal(barrier, inc=1, device_id={"mp_2": lax.rem(z + o, 8)}, device_id_type=MESH)
    pl.semaphore_wait(barrier, PLANE - 1 + 7)


def soft(logits):
    exponent = jnp.exp(logits - jnp.max(logits, axis=1, keepdims=True))
    return exponent / jnp.sum(exponent, axis=1, keepdims=True)


def block_of(p):
    return pl.ds(lax.rem(p, 8) * 4, 4), pl.ds(pl.multiple_of(lax.div(p, 8) * ROWS, ROWS), ROWS)


def forward_kernel(
    tids, logits, sp, kw, vw, pp, sel,
    mix_t, spv, w, tb, tt, out,
    load_sem, own_sem, xs, xr, zs, zr, ys, yr, us, ur, ts, tr, ps, pr,
):
    a, c, x, y, z = here()
    d = a * 2 + c
    me = plane_index(a, c, x, y)
    loads = (
        pltpu.make_async_copy(sp.at[pl.ds(d * ROWS, ROWS)], spv, load_sem.at[0]),
        pltpu.make_async_copy(kw, w.at[pl.ds(0, COLS)], load_sem.at[1]),
        pltpu.make_async_copy(vw, w.at[pl.ds(COLS, COLS)], load_sem.at[2]),
    )
    for load in loads:
        load.start()
    tt[me] = jnp.full((8, 128), tids[x * 32 + y * 8 + z], jnp.int32).astype(F32)
    tile = jnp.concatenate([soft(logits[...]).astype(BF16).astype(F32)] * ROWS, axis=0)
    row = lax.broadcasted_iota(jnp.int32, (128, 128), 0)
    loads[0].wait()
    total = jnp.zeros((COLS, 128), F32)
    for r in range(ROWS):
        weights = jnp.where(row // NTASK == r, tile, 0.0).astype(BF16)
        total += lax.dot_general(spv[r], weights, (((1,), (1,)), ((), ())), preferred_element_type=F32)
    mix_t[x, y, z] = total.astype(BF16)
    greet(me, z)

    over = push(mix_t.at[x, y, z], mix_t.at[x, y, z], xs, xr, {"mp_0": 1 - x})
    over.start()

    def task_push(o):
        return push(tt.at[me], tt.at[me], ts.at[o], tr.at[o], plane_device(lax.rem(me + o, PLANE)))

    def task_start(o, carry):
        task_push(o).start()
        return carry

    lax.fori_loop(1, PLANE, task_start, 0)
    push(mix_t.at[1 - x, y, z], mix_t.at[1 - x, y, z], xs, xr, {"mp_0": 1 - x}).wait_recv()
    z_pushes = [
        push(mix_t.at[:, y, z], mix_t.at[:, y, z], zs.at[o], zr.at[o], {"mp_2": lax.rem(z + o, 8)}) for o in range(1, 8)
    ]
    for one in z_pushes:
        one.start()
    for o in range(1, 8):
        source = lax.rem(z - o + 8, 8)
        push(mix_t.at[:, y, source], mix_t.at[:, y, source], zs.at[o], zr.at[o], {"mp_2": source}).wait_recv()
    up, down = lax.rem(y + 1, 4), lax.rem(y + 3, 4)
    y_pushes = [
        push(mix_t.at[:, y], mix_t.at[:, y], ys.at[0], yr.at[0], {"mp_1": up}),
        push(mix_t.at[:, y], mix_t.at[:, y], ys.at[1], yr.at[1], {"mp_1": down}),
    ]
    for one in y_pushes:
        one.start()
    loads[1].wait()
    loads[2].wait()

    def project(at, total):
        for half in range(2):
            columns = pl.ds(pl.multiple_of(half * 2048 + at * 512, 512), 512)
            total += jnp.dot(w[:, columns], mix_t[half, at].reshape(512, 128), preferred_element_type=F32)
        return total

    total = project(y, jnp.zeros((128, 128), F32))
    push(mix_t.at[:, down], mix_t.at[:, down], ys.at[0], yr.at[0], {"mp_1": down}).wait_recv()
    onward = push(mix_t.at[0, down], mix_t.at[0, down], ys.at[2], yr.at[2], {"mp_1": up})
    onward.start()
    push(mix_t.at[:, up], mix_t.at[:, up], ys.at[1], yr.at[1], {"mp_1": up}).wait_recv()
    back = push(mix_t.at[1, up], mix_t.at[1, up], ys.at[3], yr.at[3], {"mp_1": down})
    back.start()
    total = project(up, project(down, total))
    across = lax.rem(y + 2, 4)
    push(mix_t.at[0, across], mix_t.at[0, across], ys.at[2], yr.at[2], {"mp_1": down}).wait_recv()
    push(mix_t.at[1, across], mix_t.at[1, across], ys.at[3], yr.at[3], {"mp_1": up}).wait_recv()
    total = project(across, total)

    tb[z] = total.astype(BF16)
    u_pushes = [push(tb.at[z], tb.at[z], us.at[o], ur.at[o], {"mp_2": lax.rem(z + o, 8)}) for o in range(1, 8)]
    for one in u_pushes:
        one.start()

    def task_wait(o, carry):
        source = lax.rem(me - o + PLANE, PLANE)
        push(tt.at[source], tt.at[source], ts.at[o], tr.at[o], plane_device(source)).wait_recv()
        return carry

    lax.fori_loop(1, PLANE, task_wait, 0)
    lane = lax.broadcasted_iota(jnp.int32, (ROWS, 128), 1)
    prompt_row = lax.broadcasted_iota(jnp.int32, (ROWS, 128), 0)
    lane_task = (lane % NTASK).astype(F32)

    def select(p, carry):
        task = jnp.concatenate([tt[p], tt[p]], axis=0)
        hit = jnp.where((lane // NTASK == prompt_row) & (task == lane_task), 1.0, 0.0)
        sel[pl.ds(pl.multiple_of(p * ROWS, ROWS), ROWS), :] = hit.astype(BF16)
        return carry

    lax.fori_loop(0, PLANE, select, 0)
    for o in range(1, 8):
        source = lax.rem(z - o + 8, 8)
        push(tb.at[source], tb.at[source], us.at[o], ur.at[o], {"mp_2": source}).wait_recv()
    for i in range(4):
        for kv in range(2):
            part = slice(kv * COLS, (kv + 1) * COLS)
            head = jnp.concatenate([tb[2 * i, part, :], tb[2 * i + 1, part, :]], axis=0)
            picked = lax.dot_general(sel[...], head, (((1,), (1,)), ((), ())), preferred_element_type=F32)
            out[:, i, kv] = picked.astype(BF16).reshape(PLANE, ROWS, DH)

    heads, rows = block_of(me)
    own = pltpu.make_async_copy(out.at[me], pp.at[heads, :, rows, :], own_sem)
    own.start()

    def pair_push(o):
        p = lax.rem(me + o, PLANE)
        return push(out.at[p], pp.at[heads, :, rows, :], ps.at[o], pr.at[o], plane_device(p))

    def pair_start(o, carry):
        pair_push(o).start()
        return carry

    lax.fori_loop(1, PLANE, pair_start, 0)

    def pair_wait(o, carry):
        source = lax.rem(me - o + PLANE, PLANE)
        source_heads, source_rows = block_of(source)
        landing = pp.at[source_heads, :, source_rows, :]
        push(out.at[source], landing, ps.at[o], pr.at[o], plane_device(source)).wait_recv()
        return carry

    lax.fori_loop(1, PLANE, pair_wait, 0)
    own.wait()

    def sent_wait(o, carry):
        pair_push(o).wait_send()
        task_push(o).wait_send()
        return carry

    lax.fori_loop(1, PLANE, sent_wait, 0)
    for one in [over, onward, back, *z_pushes, *y_pushes, *u_pushes]:
        one.wait_send()


def forward(task_ids, task_logits, sp, kw, vw):
    any_space = pl.BlockSpec(memory_space=pl.ANY)
    vmem = pl.BlockSpec(memory_space=pltpu.VMEM)
    dma = pltpu.SemaphoreType.DMA
    return pl.pallas_call(
        forward_kernel,
        out_shape=(
            jax.ShapeDtypeStruct((HEADS, 2, PTOK, DH), BF16),
            jax.ShapeDtypeStruct((PLANE * ROWS, 128), BF16),
        ),
        in_specs=[pl.BlockSpec(memory_space=pltpu.SMEM), vmem, any_space, any_space, any_space],
        out_specs=(any_space, vmem),
        scratch_shapes=[
            pltpu.VMEM((2, 4, 8, COLS, 128), BF16),
            pltpu.VMEM((ROWS, COLS, NSRC), BF16),
            pltpu.VMEM((2 * COLS, D), BF16),
            pltpu.VMEM((8, 128, 128), BF16),
            pltpu.VMEM((PLANE, 8, 128), F32),
            pltpu.VMEM((PLANE, 4, 2, ROWS, DH), BF16),
            dma((3,)), dma, dma, dma, dma((8,)), dma((8,)), dma((4,)), dma((4,)), dma((8,)), dma((8,)),
            dma((PLANE,)), dma((PLANE,)), dma((PLANE,)), dma((PLANE,)),
        ],
        compiler_params=pltpu.CompilerParams(collective_id=0, has_side_effects=True),
        name="prompt_forward",
    )(task_ids, task_logits, sp, kw, vw)


HEADS_STEP = 4


def attention_kernel(q_ref, k_ref, v_ref, c_ref, pp_ref, o_ref, g_ref):
    scale = DH ** (-0.5)
    nt = (((1,), (1,)), ((), ()))
    tn = (((0,), (0,)), ((), ()))
    column = lax.broadcasted_iota(jnp.int32, (SEQ, SEQ), 1)
    position = lax.broadcasted_iota(jnp.int32, (SEQ, SEQ), 0)
    visible = column <= position
    for h in range(HEADS_STEP):
        lanes = slice(h * DH, (h + 1) * DH)
        q, k, v, cot = q_ref[:, lanes], k_ref[:, lanes], v_ref[:, lanes], c_ref[:, lanes]
        pk, pv = pp_ref[h, 0], pp_ref[h, 1]
        ps = lax.dot_general(q, pk, nt, preferred_element_type=F32) * scale
        ss = lax.dot_general(q, k, nt, preferred_element_type=F32) * scale
        ss = jnp.where(visible, ss, -1e30)
        top = jnp.maximum(jnp.max(ps, axis=1, keepdims=True), jnp.max(ss, axis=1, keepdims=True))
        pe, se = jnp.exp(ps - top), jnp.exp(ss - top)
        inverse = 1.0 / (jnp.sum(pe, axis=1, keepdims=True) + jnp.sum(se, axis=1, keepdims=True))
        pa, sa = pe * inverse, se * inverse
        par, sar = pa.astype(BF16), sa.astype(BF16)
        attended = jnp.dot(par, pv, preferred_element_type=F32) + jnp.dot(sar, v, preferred_element_type=F32)
        o_ref[:, lanes] = attended.astype(BF16)
        pg = lax.dot_general(cot, pv, nt, preferred_element_type=F32)
        sg = lax.dot_general(cot, v, nt, preferred_element_type=F32)
        inner = jnp.sum(pa * pg, axis=1, keepdims=True) + jnp.sum(sa * sg, axis=1, keepdims=True)
        gs = (pa * (pg - inner)).astype(BF16)
        g_ref[h, 0] = (lax.dot_general(gs, q, tn, preferred_element_type=F32) * scale).astype(BF16)
        g_ref[h, 1] = lax.dot_general(par, cot, tn, preferred_element_type=F32).astype(BF16)


def attention(q, k, v, cot, pp):
    wide = pl.BlockSpec((SEQ, HEADS_STEP * DH), lambda i: (0, i))
    pair = pl.BlockSpec((HEADS_STEP, 2, PTOK, DH), lambda i: (i, 0, 0, 0))
    return pl.pallas_call(
        attention_kernel,
        grid=(HEADS // HEADS_STEP,),
        out_shape=(
            jax.ShapeDtypeStruct((SEQ, D), BF16),
            jax.ShapeDtypeStruct((HEADS, 2, PTOK, DH), BF16),
        ),
        in_specs=[wide, wide, wide, wide, pair],
        out_specs=(wide, pair),
        name="prompt_attention",
    )(q, k, v, cot, pp)


def backward_kernel(
    logits, sel, sp, kw, vw, gg, source_grad, logits_grad,
    spv, w, rg, gz, rz, rt, ry, t2, rz2, sx, rx, wslot, wz,
    load_sem, own_sem, ps, pr, us, ur, ys, yr, zs, zr, xs, xr, ws, wr, vs, vr,
):
    a, c, x, y, z = here()
    d = a * 2 + c
    me = plane_index(a, c, x, y)
    tn = (((0,), (0,)), ((), ()))
    loads = (
        pltpu.make_async_copy(sp.at[pl.ds(d * ROWS, ROWS)], spv, load_sem.at[0]),
        pltpu.make_async_copy(kw, w.at[pl.ds(0, COLS)], load_sem.at[1]),
        pltpu.make_async_copy(vw, w.at[pl.ds(COLS, COLS)], load_sem.at[2]),
    )
    for load in loads:
        load.start()
    heads, rows = block_of(me)
    own = pltpu.make_async_copy(gg.at[heads, :, rows, :], rg.at[me], own_sem)
    own.start()
    greet(me, z)

    def pair_push(o):
        p = lax.rem(me + o, PLANE)
        p_heads, p_rows = block_of(p)
        return push(gg.at[p_heads, :, p_rows, :], rg.at[me], ps.at[o], pr.at[o], plane_device(p))

    def pair_start(o, carry):
        pair_push(o).start()
        return carry

    lax.fori_loop(1, PLANE, pair_start, 0)

    def pair_wait(o, carry):
        source = lax.rem(me - o + PLANE, PLANE)
        push(gg.at[heads, :, rows, :], rg.at[source], ps.at[o], pr.at[o], plane_device(source)).wait_recv()
        return carry

    lax.fori_loop(1, PLANE, pair_wait, 0)
    own.wait()
    for i in range(4):
        for kv in range(2):
            arrived = rg[:, i, kv].reshape(PLANE * ROWS, DH)
            summed = lax.dot_general(arrived, sel[...], tn, preferred_element_type=F32).astype(BF16)
            gz[2 * i, kv * COLS : (kv + 1) * COLS, :] = summed[:COLS]
            gz[2 * i + 1, kv * COLS : (kv + 1) * COLS, :] = summed[COLS:]

    u_pushes = []
    for o in range(1, 8):
        other = lax.rem(z + o, 8)
        u_pushes.append(push(gz.at[other], rz.at[o], us.at[o], ur.at[o], {"mp_2": other}))
    for one in u_pushes:
        one.start()
    loads[1].wait()
    loads[2].wait()
    grad = gz[z].astype(F32)
    for o in range(1, 8):
        push(gz.at[z], rz.at[o], us.at[o], ur.at[o], {"mp_2": lax.rem(z - o + 8, 8)}).wait_recv()
        grad += rz[o].astype(F32)
    grad_high = grad.astype(BF16)
    grad_low = (grad - grad_high.astype(F32)).astype(BF16)

    def row_terms(at):
        for half in range(2):
            columns = pl.ds(pl.multiple_of(half * 2048 + at * 512, 512), 512)
            part = w[:, columns]
            terms = lax.dot_general(part, grad_high, tn, preferred_element_type=F32)
            terms += lax.dot_general(part, grad_low, tn, preferred_element_type=F32)
            rt[at, half] = terms.astype(BF16).reshape(8, COLS, 128)

    y_pushes = []
    for o in (2, 1, 3):
        other = lax.rem(y + o, 4)
        row_terms(other)
        one = push(rt.at[other], ry.at[o], ys.at[o], yr.at[o], {"mp_1": other})
        one.start()
        y_pushes.append(one)
    row_terms(y)
    for o in range(1, 4):
        push(rt.at[y], ry.at[o], ys.at[o], yr.at[o], {"mp_1": lax.rem(y - o + 4, 4)}).wait_recv()
    for half in range(2):
        four = rt[y, half].astype(F32)
        for o in range(1, 4):
            four += ry[o, half].astype(F32)
        t2[:, half] = four.astype(BF16)
    z_pushes = []
    for o in range(1, 8):
        other = lax.rem(z + o, 8)
        one = push(t2.at[other], rz2.at[o], zs.at[o], zr.at[o], {"mp_2": other})
        one.start()
        z_pushes.append(one)
    eight = t2[z].astype(F32)
    for o in range(1, 8):
        push(t2.at[z], rz2.at[o], zs.at[o], zr.at[o], {"mp_2": lax.rem(z - o + 8, 8)}).wait_recv()
        eight += rz2[o].astype(F32)
    sx[...] = eight
    over = push(sx.at[1 - x], rx, xs, xr, {"mp_0": 1 - x})
    over.start()
    mix = soft(logits[...])
    loads[0].wait()
    push(sx.at[1 - x], rx, xs, xr, {"mp_0": 1 - x}).wait_recv()
    mixture_grad = sx[x] + rx[...]

    flipped = mixture_grad.T
    part = jnp.zeros((NTASK, NSRC), F32)
    for r in range(ROWS):
        part += jnp.dot(
            flipped[r * NTASK : (r + 1) * NTASK], spv[r].astype(F32), precision=HIGH, preferred_element_type=F32
        )
    wslot[me] = part

    def weight_push(o):
        return push(wslot.at[me], wslot.at[me], ws.at[o], wr.at[o], plane_device(lax.rem(me + o, PLANE)))

    def weight_start(o, carry):
        weight_push(o).start()
        return carry

    lax.fori_loop(1, PLANE, weight_start, 0)
    tile = jnp.concatenate([mix] * ROWS, axis=0)
    lane = lax.broadcasted_iota(jnp.int32, (COLS, 128), 1)
    for r in range(ROWS):
        chosen = jnp.where(lane // NTASK == r, mixture_grad, 0.0)
        source_grad[r] = jnp.dot(chosen, tile, precision=HIGH, preferred_element_type=F32)

    def weight_wait(o, carry):
        source = lax.rem(me - o + PLANE, PLANE)
        push(wslot.at[source], wslot.at[source], ws.at[o], wr.at[o], plane_device(source)).wait_recv()
        return carry

    lax.fori_loop(1, PLANE, weight_wait, 0)
    wz[z] = jnp.sum(wslot[...], axis=0)
    v_pushes = [push(wz.at[z], wz.at[z], vs.at[o], vr.at[o], {"mp_2": lax.rem(z + o, 8)}) for o in range(1, 8)]
    for one in v_pushes:
        one.start()
    for o in range(1, 8):
        source = lax.rem(z - o + 8, 8)
        push(wz.at[source], wz.at[source], vs.at[o], vr.at[o], {"mp_2": source}).wait_recv()
    weight_grad = jnp.sum(wz[...], axis=0)
    logits_grad[...] = mix * (weight_grad - jnp.sum(mix * weight_grad, axis=1, keepdims=True))

    def sent_wait(o, carry):
        pair_push(o).wait_send()
        weight_push(o).wait_send()
        return carry

    lax.fori_loop(1, PLANE, sent_wait, 0)
    for one in [over, *u_pushes, *y_pushes, *z_pushes, *v_pushes]:
        one.wait_send()


def backward(task_logits, sel, sp, kw, vw, gg):
    any_space = pl.BlockSpec(memory_space=pl.ANY)
    vmem = pl.BlockSpec(memory_space=pltpu.VMEM)
    dma = pltpu.SemaphoreType.DMA
    return pl.pallas_call(
        backward_kernel,
        out_shape=(
            jax.ShapeDtypeStruct((ROWS, COLS, NSRC), F32),
            jax.ShapeDtypeStruct((NTASK, NSRC), F32),
        ),
        in_specs=[vmem, vmem, any_space, any_space, any_space, any_space],
        out_specs=(vmem, vmem),
        scratch_shapes=[
            pltpu.VMEM((ROWS, COLS, NSRC), BF16),
            pltpu.VMEM((2 * COLS, D), BF16),
            pltpu.VMEM((PLANE, 4, 2, ROWS, DH), BF16),
            pltpu.VMEM((8, 128, 128), BF16),
            pltpu.VMEM((8, 128, 128), BF16),
            pltpu.VMEM((4, 2, 8, COLS, 128), BF16),
            pltpu.VMEM((4, 2, 8, COLS, 128), BF16),
            pltpu.VMEM((8, 2, COLS, 128), BF16),
            pltpu.VMEM((8, 2, COLS, 128), BF16),
            pltpu.VMEM((2, COLS, 128), F32),
            pltpu.VMEM((COLS, 128), F32),
            pltpu.VMEM((PLANE, NTASK, NSRC), F32),
            pltpu.VMEM((8, NTASK, NSRC), F32),
            dma((3,)), dma, dma((PLANE,)), dma((PLANE,)), dma((8,)), dma((8,)), dma((4,)), dma((4,)),
            dma((8,)), dma((8,)), dma, dma, dma((PLANE,)), dma((PLANE,)), dma((8,)), dma((8,)),
        ],
        compiler_params=pltpu.CompilerParams(collective_id=1, has_side_effects=True),
        name="prompt_backward",
    )(task_logits, sel, sp, kw, vw, gg)


def on_device(source_prompts, task_logits, task_ids, key_weight, value_weight, queries, keys, values, cotangent):
    sp = source_prompts.transpose(1, 2, 0)
    kw, vw = key_weight.T, value_weight.T
    pp, sel = forward(task_ids, task_logits, sp, kw, vw)
    attended, gg = attention(queries[0], keys[0], values[0], cotangent[0], pp)
    source_grad, logits_grad = backward(task_logits, sel, sp, kw, vw, gg)
    return attended[None], source_grad.transpose(2, 0, 1), logits_grad


def solution(mesh):
    torus = Mesh(mesh.devices.reshape(2, 2, 2, 4, 8), AXES)
    return jax.shard_map(
        on_device,
        mesh=torus,
        in_specs=(
            P(None, None, MP),
            P(),
            P(DP),
            P(None, MP),
            P(None, MP),
            P(AXES, None, None),
            P(AXES, None, None),
            P(AXES, None, None),
            P(AXES, None, None),
        ),
        out_specs=(P(AXES, None, None), P(None, DP, MP), P()),
        check_vma=False,
    )
```

```python
import functools

import jax
import jax.numpy as jnp
from jax import lax
from jax.experimental import pallas as pl
from jax.experimental.pallas import tpu as pltpu
from jax.sharding import Mesh
from jax.sharding import PartitionSpec as P

D = 4096
HEADS = 32
DH = 128
NSRC = 128
NTASK = 8
PTOK = 64
SEQ = 128
AXES = ("dp_0", "dp_1", "mp_0", "mp_1", "mp_2")
MP = ("mp_0", "mp_1", "mp_2")
DP = ("dp_0", "dp_1")
MESH = pl.DeviceIdType.MESH
ROWS = 16
COLS = 64
PLANE = 32
F32 = jnp.float32
BF16 = jnp.bfloat16
HIGH = lax.Precision.HIGHEST


def here():
    return tuple(lax.axis_index(name) for name in AXES)


def push(src, dst, sent, landed, device):
    return pltpu.make_async_remote_copy(
        src_ref=src, dst_ref=dst, send_sem=sent, recv_sem=landed, device_id=device, device_id_type=MESH
    )


def soft(logits):
    exponent = jnp.exp(logits - jnp.max(logits, axis=1, keepdims=True))
    return exponent / jnp.sum(exponent, axis=1, keepdims=True)


NN = (((1,), (0,)), ((), ()))
NT = (((1,), (1,)), ((), ()))
TN = (((0,), (0,)), ((), ()))
SCALE = DH ** (-0.5)
HOPS = (0, 1, 3, 2)
PRE_HEADS = 2
MID_HEADS = 2
POST_HEADS = 2


def dot(a, b, dims=NN):
    return lax.dot_general(a, b, dims, preferred_element_type=F32)


def kernel(
    tids, logits, sp, kw, vw, queries, keys, values, cotangent,
    attended, source_grad, logits_grad,
    spv, w, qv, kv, vv, cv, mix_t, tb, tt, sel, out, pp, stat, self_e, pat, gg, rg, gz, rz, rt, ry, t2, rz2, sx, rx,
    wslot, wz,
    load_sem, zs, zr, xs, xr, ys, yr, us, ur, ts, tr, ps, pr, gs, gr, bs, br, cs, cr, es, er, fs, fr, ws, wr, vs, vr,
):
    a, c, x, y, z = here()
    d, g = a * 2 + c, x * 4 + y
    me = d * 8 + g
    pair = lax.div(z, 2)
    barrier = pltpu.get_barrier_semaphore()

    def device(d_to, g_to):
        return {
            "dp_0": lax.div(d_to, 2), "dp_1": lax.rem(d_to, 2), "mp_0": lax.div(g_to, 4), "mp_1": lax.rem(g_to, 4),
        }

    def along(o, n, at):
        return lax.rem(at + o + n, n)

    def around(m):
        k, dd = lax.div(m, 4), lax.rem(m, 4)
        return along(dd, 4, d), along(-k, 8, g), along(-dd, 4, d), along(k, 8, g)

    def plane(body):
        lax.fori_loop(1, PLANE, lambda m, carry: (body(m), carry)[1], 0)

    def rows(quarter):
        return pl.ds(pl.multiple_of(quarter * ROWS, ROWS), ROWS)

    def signal(m):
        d_to, g_to, _, _ = around(m)
        pl.semaphore_signal(barrier, inc=1, device_id=device(d_to, g_to), device_id_type=MESH)

    plane(signal)
    for o in range(1, 8):
        pl.semaphore_signal(barrier, inc=1, device_id={"mp_2": along(o, 8, z)}, device_id_type=MESH)
    loads = [
        pltpu.make_async_copy(sp.at[pl.ds(d * ROWS, ROWS)], spv, load_sem.at[0]),
        pltpu.make_async_copy(queries, qv, load_sem.at[1]),
        pltpu.make_async_copy(keys, kv, load_sem.at[2]),
        pltpu.make_async_copy(cotangent, cv, load_sem.at[3]),
        pltpu.make_async_copy(values, vv, load_sem.at[4]),
        pltpu.make_async_copy(kw, w.at[pl.ds(0, COLS)], load_sem.at[5]),
        pltpu.make_async_copy(vw, w.at[pl.ds(COLS, COLS)], load_sem.at[6]),
    ]
    for load in loads:
        load.start()
    tt[me] = jnp.full((8, 128), tids[x * 32 + y * 8 + z], jnp.int32).astype(F32)
    tile = jnp.concatenate([soft(logits[...]).astype(BF16).astype(F32)] * ROWS, axis=0)
    row = lax.broadcasted_iota(jnp.int32, (128, 128), 0)
    loads[0].wait()
    total = jnp.zeros((COLS, 128), F32)
    for r in range(ROWS):
        weights = jnp.where(row // NTASK == r, tile, 0.0).astype(BF16)
        total += dot(spv[r], weights, NT)
    mix_t[x, y, z] = total.astype(BF16)
    pl.semaphore_wait(barrier, PLANE - 1 + 7)

    sends = []

    def send(src, dst, sent, landed, to):
        one = push(src, dst, sent, landed, to)
        one.start()
        sends.append(one)

    own = mix_t.at[x, y, z]
    for o in (1, 7, 2, 6, 3, 5, 4):
        send(own, own, zs.at[o], zr.at[o], {"mp_2": along(o, 8, z)})

    def task_push(m):
        d_to, g_to, d_from, g_from = around(m)
        return push(tt.at[me], tt.at[me], ts.at[m], tr.at[m], device(d_to, g_to))

    plane(lambda m: task_push(m).start())

    def pre(first, count):
        masked = lax.broadcasted_iota(jnp.int32, (SEQ, SEQ), 0) > lax.broadcasted_iota(jnp.int32, (SEQ, SEQ), 1)

        def step(n, carry):
            for e in range(PRE_HEADS):
                h = first + n * PRE_HEADS + e
                lanes = pl.ds(pl.multiple_of(h * DH, DH), DH)
                scores = dot(kv[:, lanes], qv[:, lanes], NT) * SCALE
                scores = jnp.where(masked, -1e30, scores)
                top = jnp.max(scores, axis=0, keepdims=True)
                exponent = jnp.exp(scores - top)
                grad = dot(vv[:, lanes], cv[:, lanes], NT)
                self_e[h] = exponent
                stat[h, 0:1] = top
                stat[h, 1:2] = jnp.sum(exponent, axis=0, keepdims=True)
                stat[h, 2:3] = jnp.sum(exponent * grad, axis=0, keepdims=True)
            return carry

        lax.fori_loop(0, count // PRE_HEADS, step, 0)

    for load in loads[1:5]:
        load.wait()
    pre(0, 10)
    for o in (1, 7, 2, 6, 3, 5, 4):
        source = along(-o, 8, z)
        push(mix_t.at[x, y, source], mix_t.at[x, y, source], zs.at[o], zr.at[o], {"mp_2": source}).wait_recv()
    up, down, across = along(1, 4, y), along(-1, 4, y), along(2, 4, y)
    other = 1 - x

    def y_start(half, n):
        block = mix_t.at[half, y]
        send(block, block, ys.at[n, 0], yr.at[n, 0], {"mp_1": up})
        send(block, block, ys.at[n, 1], yr.at[n, 1], {"mp_1": down})

    def y_relay(half, n):
        block, part = mix_t.at[half, down], mix_t.at[half, down, pl.ds(0, 4)]
        push(block, block, ys.at[n, 0], yr.at[n, 0], {"mp_1": down}).wait_recv()
        send(part, part, ys.at[n, 2], yr.at[n, 2], {"mp_1": up})
        block, part = mix_t.at[half, up], mix_t.at[half, up, pl.ds(4, 4)]
        push(block, block, ys.at[n, 1], yr.at[n, 1], {"mp_1": up}).wait_recv()
        send(part, part, ys.at[n, 3], yr.at[n, 3], {"mp_1": down})

    def y_end(half, n):
        part = mix_t.at[half, across, pl.ds(0, 4)]
        push(part, part, ys.at[n, 2], yr.at[n, 2], {"mp_1": down}).wait_recv()
        part = mix_t.at[half, across, pl.ds(4, 4)]
        push(part, part, ys.at[n, 3], yr.at[n, 3], {"mp_1": up}).wait_recv()

    def project(half, at):
        columns = pl.ds(pl.multiple_of(half * 2048 + at * 512, 512), 512)
        return dot(w[:, columns], mix_t[half, at].reshape(512, 128))

    y_start(x, 0)
    send(mix_t.at[x, y], mix_t.at[x, y], xs, xr, {"mp_0": other})
    for load in loads[5:]:
        load.wait()
    pre(10, 8)
    total = project(x, y)
    push(mix_t.at[other, y], mix_t.at[other, y], xs, xr, {"mp_0": other}).wait_recv()
    y_start(other, 1)
    y_relay(x, 0)
    total += project(other, y) + project(x, down) + project(x, up)

    def task_wait(m):
        d_to, g_to, d_from, g_from = around(m)
        slot = tt.at[d_from * 8 + g_from]
        push(slot, slot, ts.at[m], tr.at[m], device(d_from, g_from)).wait_recv()

    plane(task_wait)
    lane = lax.broadcasted_iota(jnp.int32, (ROWS, 128), 1)
    prompt_row = lax.broadcasted_iota(jnp.int32, (ROWS, 128), 0)
    lane_task = (lane % NTASK).astype(F32)

    def select(p, carry):
        task = jnp.concatenate([tt[p], tt[p]], axis=0)
        hit = jnp.where((lane // NTASK == prompt_row) & (task == lane_task), 1.0, 0.0)
        sel[rows(p), :] = hit.astype(BF16)
        return carry

    lax.fori_loop(0, PLANE, select, 0)
    y_relay(other, 1)
    y_end(x, 0)
    total += project(other, down) + project(other, up) + project(x, across)
    y_end(other, 1)
    total += project(other, across)

    tb[z] = total.astype(BF16)
    mate = pair * 2 + 1 - lax.rem(z, 2)

    def u_send(to):
        o = along(to - z, 8, 0)
        send(tb.at[z], tb.at[z], us.at[o], ur.at[o], {"mp_2": to})

    def u_wait(source):
        o = along(z - source, 8, 0)
        push(tb.at[source], tb.at[source], us.at[o], ur.at[o], {"mp_2": source}).wait_recv()

    u_send(mate)
    for hop in HOPS[1:]:
        for side in range(2):
            u_send(along(-hop, 4, pair) * 2 + side)

    def pair_push(j, i, m):
        d_to, g_to, d_from, g_from = around(m)
        return push(
            out.at[i, d_to * 8 + g_to], pp.at[i, g, :, rows(d), :], ps.at[j, m], pr.at[j, m], device(d_to, g_to)
        )

    pieces = [along(hop, 4, pair) for hop in HOPS]
    for j, i in enumerate(pieces):
        if j == 0:
            pre(18, 4)
            u_wait(mate)
        else:
            u_wait(2 * i)
            u_wait(2 * i + 1)
        for which in range(2):
            part = slice(which * COLS, (which + 1) * COLS)
            table = jnp.concatenate([tb[2 * i, part, :], tb[2 * i + 1, part, :]], axis=0)
            out[i, :, which] = dot(sel[...], table, NT).astype(BF16).reshape(PLANE, ROWS, DH)
        plane(functools.partial(lambda j, i, m: pair_push(j, i, m).start(), j, i))
        for which in range(2):
            pp[i, g, which, rows(d), :] = out[i, me, which]
    pre(22, 10)

    def mid(j, i, k, skip_own):
        g_here = along(k, 8, g)
        for dd in range(1 if skip_own else 0, 4):
            d_from = along(-dd, 4, d)
            landing = pp.at[i, g_here, :, rows(d_from), :]
            m = k * 4 + dd
            push(landing, landing, ps.at[j, m], pr.at[j, m], device(d_from, g_here)).wait_recv()
        return g_here

    def head(i, g_here):
        h = g_here * 4 + i
        lanes = pl.ds(pl.multiple_of(h * DH, DH), DH)
        q, cot = qv[:, lanes], cv[:, lanes]
        scores = dot(pp[i, g_here, 0], q, NT) * SCALE
        grad = dot(pp[i, g_here, 1], cot, NT)
        self_top = stat[h, 0:1]
        top = jnp.maximum(jnp.max(scores, axis=0, keepdims=True), self_top)
        exponent = jnp.exp(scores - top)
        shrink = jnp.exp(self_top - top)
        inverse = 1.0 / (shrink * stat[h, 1:2] + jnp.sum(exponent, axis=0, keepdims=True))
        attention = exponent * inverse
        self_scale = shrink * inverse
        stat[h, 3:4] = self_scale
        rounded = attention.astype(BF16)
        pat[h] = rounded
        inner = self_scale * stat[h, 2:3] + jnp.sum(attention * grad, axis=0, keepdims=True)
        grad_scores = (attention * (grad - inner)).astype(BF16)
        gg[i, g_here, 0] = (dot(grad_scores, q) * SCALE).astype(BF16)
        gg[i, g_here, 1] = dot(rounded, cot).astype(BF16)

    def grad_push(j, i, k, dd):
        m = k * 4 + dd
        d_to, g_here = along(dd, 4, d), along(k, 8, g)
        return push(
            gg.at[i, g_here, :, rows(d_to), :], rg.at[i, me], gs.at[j, m], gr.at[j, m], device(d_to, g_here)
        )

    def mid_step(j, i, ks, skip_own):
        groups = [mid(j, i, k, skip_own and n == 0) for n, k in enumerate(ks)]
        for g_here in groups:
            head(i, g_here)
        for n, k in enumerate(ks):
            for dd in range(1 if skip_own and n == 0 else 0, 4):
                grad_push(j, i, k, dd).start()

    for j, i in enumerate(pieces):
        mid_step(j, i, list(range(MID_HEADS)), True)
        rg[i, me] = gg[i, g, :, rows(d), :]

        def later(n, carry, j=j, i=i):
            mid_step(j, i, [n * MID_HEADS + e for e in range(MID_HEADS)], False)
            return carry

        lax.fori_loop(1, 8 // MID_HEADS, later, 0)

    def post(first, count):
        def step(n, carry):
            for e in range(POST_HEADS):
                h = first + n * POST_HEADS + e
                lanes = pl.ds(pl.multiple_of(h * DH, DH), DH)
                self_part = (self_e[h] * stat[h, 3:4]).astype(BF16)
                prompt_values = pp[lax.rem(h, 4), lax.div(h, 4), 1]
                summed = dot(self_part, vv[:, lanes], TN) + dot(pat[h], prompt_values, TN)
                attended[:, lanes] = summed.astype(BF16)
            return carry

        lax.fori_loop(0, count // POST_HEADS, step, 0)

    post(0, 8)

    for j, i in enumerate(pieces):

        def grad_wait(m, j=j, i=i):
            k, dd = lax.div(m, 4), lax.rem(m, 4)
            d_from, g_from = along(-dd, 4, d), along(-k, 8, g)
            landing = rg.at[i, d_from * 8 + g_from]
            push(landing, landing, gs.at[j, m], gr.at[j, m], device(d_from, g_from)).wait_recv()

        plane(grad_wait)
        for which in range(2):
            summed = dot(rg[i, :, which].reshape(PLANE * ROWS, DH), sel[...], TN).astype(BF16)
            part = slice(which * COLS, (which + 1) * COLS)
            gz[2 * i, part, :] = summed[:COLS]
            gz[2 * i + 1, part, :] = summed[COLS:]
        for to in (mate,) if j == 0 else (2 * i, 2 * i + 1):
            o = along(to - z, 8, 0)
            send(gz.at[to], rz.at[o], bs.at[o], br.at[o], {"mp_2": to})
    post(8, 8)
    grad = gz[z].astype(F32)
    for o in (1, 7, 2, 6, 3, 5, 4):
        push(gz.at[z], rz.at[o], bs.at[o], br.at[o], {"mp_2": along(-o, 8, z)}).wait_recv()
        grad += rz[o].astype(F32)
    grad_high = grad.astype(BF16)
    grad_low = (grad - grad_high.astype(F32)).astype(BF16)
    grad_both = jnp.concatenate([grad_high, grad_low], axis=1)

    def row_terms(half, at):
        columns = pl.ds(pl.multiple_of(half * 2048 + at * 512, 512), 512)
        terms = dot(w[:, columns], grad_both, TN)
        rt[half, at] = (terms[:, :128] + terms[:, 128:]).astype(BF16).reshape(8, COLS, 128)

    halves = (other, x)
    for n, half in enumerate(halves):
        for o in (2, 1, 3):
            to = along(o, 4, y)
            row_terms(half, to)
            send(rt.at[half, to], ry.at[n, o], cs.at[n, o], cr.at[n, o], {"mp_1": to})
        row_terms(half, y)

    def y_sum(n, half):
        four = rt[half, y].astype(F32)
        for o in (1, 3, 2):
            push(rt.at[half, y], ry.at[n, o], cs.at[n, o], cr.at[n, o], {"mp_1": along(-o, 4, y)}).wait_recv()
            four += ry[n, o].astype(F32)
        t2[n] = four.astype(BF16)
        for o in (1, 7, 2, 6, 3, 5, 4):
            to = along(o, 8, z)
            send(t2.at[n, to], rz2.at[n, o], es.at[n, o], er.at[n, o], {"mp_2": to})

    def z_sum(n):
        eight = t2[n, z].astype(F32)
        for o in (1, 7, 2, 6, 3, 5, 4):
            push(t2.at[n, z], rz2.at[n, o], es.at[n, o], er.at[n, o], {"mp_2": along(-o, 8, z)}).wait_recv()
            eight += rz2[n, o].astype(F32)
        return eight

    post(16, 12)
    y_sum(0, other)
    y_sum(1, x)
    sx[...] = z_sum(0)
    send(sx, rx, fs, fr, {"mp_0": other})
    post(28, 4)
    mix = soft(logits[...])
    mine = z_sum(1)
    push(sx, rx, fs, fr, {"mp_0": other}).wait_recv()
    mixture_grad = mine + rx[...]

    flipped = mixture_grad.T
    part = jnp.zeros((NTASK, NSRC), F32)
    for r in range(ROWS):
        part += jnp.dot(
            flipped[r * NTASK : (r + 1) * NTASK], spv[r].astype(F32), precision=HIGH, preferred_element_type=F32
        )
    wslot[me] = part

    def weight_push(m):
        d_to, g_to, d_from, g_from = around(m)
        return push(wslot.at[me], wslot.at[me], ws.at[m], wr.at[m], device(d_to, g_to))

    plane(lambda m: weight_push(m).start())
    tile = jnp.concatenate([mix] * ROWS, axis=0)
    lane = lax.broadcasted_iota(jnp.int32, (COLS, 128), 1)
    for r in range(ROWS):
        chosen = jnp.where(lane // NTASK == r, mixture_grad, 0.0)
        source_grad[r] = jnp.dot(chosen, tile, precision=HIGH, preferred_element_type=F32)

    def weight_wait(m):
        d_to, g_to, d_from, g_from = around(m)
        slot = wslot.at[d_from * 8 + g_from]
        push(slot, slot, ws.at[m], wr.at[m], device(d_from, g_from)).wait_recv()

    plane(weight_wait)
    wz[z] = jnp.sum(wslot[...], axis=0)
    for o in range(1, 8):
        send(wz.at[z], wz.at[z], vs.at[o], vr.at[o], {"mp_2": along(o, 8, z)})
    for o in range(1, 8):
        source = along(-o, 8, z)
        push(wz.at[source], wz.at[source], vs.at[o], vr.at[o], {"mp_2": source}).wait_recv()
    weight_grad = jnp.sum(wz[...], axis=0)
    logits_grad[...] = mix * (weight_grad - jnp.sum(mix * weight_grad, axis=1, keepdims=True))

    def sent(m):
        task_push(m).wait_send()
        weight_push(m).wait_send()
        for j, i in enumerate(pieces):
            pair_push(j, i, m).wait_send()
            grad_push(j, i, lax.div(m, 4), lax.rem(m, 4)).wait_send()

    plane(sent)
    for one in sends:
        one.wait_send()


def on_device(source_prompts, task_logits, task_ids, key_weight, value_weight, queries, keys, values, cotangent):
    any_space = pl.BlockSpec(memory_space=pl.ANY)
    vmem = pl.BlockSpec(memory_space=pltpu.VMEM)
    dma = pltpu.SemaphoreType.DMA
    block = (2, 8, COLS, 128)
    attended, source_grad, logits_grad = pl.pallas_call(
        kernel,
        out_shape=(
            jax.ShapeDtypeStruct((SEQ, D), BF16),
            jax.ShapeDtypeStruct((ROWS, COLS, NSRC), F32),
            jax.ShapeDtypeStruct((NTASK, NSRC), F32),
        ),
        in_specs=[pl.BlockSpec(memory_space=pltpu.SMEM), vmem] + [any_space] * 7,
        out_specs=(vmem, vmem, vmem),
        scratch_shapes=[
            pltpu.VMEM((ROWS, COLS, NSRC), BF16),
            pltpu.VMEM((2 * COLS, D), BF16),
            *[pltpu.VMEM((SEQ, D), BF16)] * 4,
            pltpu.VMEM((2, 4, 8, COLS, 128), BF16),
            pltpu.VMEM((8, 128, 128), BF16),
            pltpu.VMEM((PLANE, 8, 128), F32),
            pltpu.VMEM((PLANE * ROWS, 128), BF16),
            pltpu.VMEM((4, PLANE, 2, ROWS, DH), BF16),
            pltpu.VMEM((4, 8, 2, PTOK, DH), BF16),
            pltpu.VMEM((HEADS, 8, SEQ), F32),
            pltpu.VMEM((HEADS, SEQ, SEQ), F32),
            pltpu.VMEM((HEADS, PTOK, SEQ), BF16),
            pltpu.VMEM((4, 8, 2, PTOK, DH), BF16),
            pltpu.VMEM((4, PLANE, 2, ROWS, DH), BF16),
            pltpu.VMEM((8, 128, 128), BF16),
            pltpu.VMEM((8, 128, 128), BF16),
            pltpu.VMEM((2, 4, 8, COLS, 128), BF16),
            pltpu.VMEM((2, 4, 8, COLS, 128), BF16),
            pltpu.VMEM(block, BF16),
            pltpu.VMEM(block, BF16),
            pltpu.VMEM((COLS, 128), F32),
            pltpu.VMEM((COLS, 128), F32),
            pltpu.VMEM((PLANE, NTASK, NSRC), F32),
            pltpu.VMEM((8, NTASK, NSRC), F32),
            dma((7,)), dma((8,)), dma((8,)), dma, dma, dma((2, 4)), dma((2, 4)), dma((8,)), dma((8,)),
            dma((PLANE,)), dma((PLANE,)), dma((4, PLANE)), dma((4, PLANE)), dma((4, PLANE)), dma((4, PLANE)),
            dma((8,)), dma((8,)), dma((2, 4)), dma((2, 4)), dma((2, 8)), dma((2, 8)), dma, dma,
            dma((PLANE,)), dma((PLANE,)), dma((8,)), dma((8,)),
        ],
        compiler_params=pltpu.CompilerParams(collective_id=0, has_side_effects=True),
        name="prompt_step",
    )(
        task_ids, task_logits, source_prompts.transpose(1, 2, 0), key_weight.T, value_weight.T,
        queries[0], keys[0], values[0], cotangent[0],
    )
    return attended[None], source_grad.transpose(2, 0, 1), logits_grad


def solution(mesh):
    torus = Mesh(mesh.devices.reshape(2, 2, 2, 4, 8), AXES)
    return jax.shard_map(
        on_device,
        mesh=torus,
        in_specs=(
            P(None, None, MP),
            P(),
            P(DP),
            P(None, MP),
            P(None, MP),
            P(AXES, None, None),
            P(AXES, None, None),
            P(AXES, None, None),
            P(AXES, None, None),
        ),
        out_specs=(P(AXES, None, None), P(None, DP, MP), P()),
        check_vma=False,
    )
```

```python
import jax
import jax.numpy as jnp
from jax import lax
from jax.experimental import pallas as pl
from jax.experimental.pallas import tpu as pltpu
from jax.sharding import Mesh
from jax.sharding import PartitionSpec as P

D = 4096
HEADS = 32
DH = 128
NSRC = 128
NTASK = 8
PTOK = 64
SEQ = 128
AXES = ("dp_0", "dp_1", "mp_0", "mp_1", "mp_2")
MP = ("mp_0", "mp_1", "mp_2")
DP = ("dp_0", "dp_1")
MESH = pl.DeviceIdType.MESH
ROWS = 16
COLS = 64
PLANE = 32
F32 = jnp.float32
BF16 = jnp.bfloat16
HIGH = lax.Precision.HIGHEST


def here():
    return tuple(lax.axis_index(name) for name in AXES)


def push(src, dst, sent, landed, device):
    return pltpu.make_async_remote_copy(
        src_ref=src, dst_ref=dst, send_sem=sent, recv_sem=landed, device_id=device, device_id_type=MESH
    )


def drain(ref, sem):
    pltpu.make_async_copy(ref, ref, sem).wait()


def soft(logits):
    exponent = jnp.exp(logits - jnp.max(logits, axis=1, keepdims=True))
    return exponent / jnp.sum(exponent, axis=1, keepdims=True)


NN = (((1,), (0,)), ((), ()))
NT = (((1,), (1,)), ((), ()))
TN = (((0,), (0,)), ((), ()))
SCALE = DH ** (-0.5)
HOPS = (1, 2, 3, 0)
RING = (1, 7, 2, 6, 3, 5, 4)
PRE_HEADS = 2
MID_HEADS = 2
POST_HEADS = 2


def dot(a, b, dims=NN):
    return lax.dot_general(a, b, dims, preferred_element_type=F32)


def kernel(
    tids, logits, sp, kw, vw, queries, keys, values, cotangent,
    attended_hbm, source_grad_hbm, logits_grad,
    spv, w, qv, kv, vv, cv, mix_t, tb, tt, sel, out, pp, stat, self_e, pat, gg, rg, gz, rz, rt, ry, t2, rz2, sx, rx,
    wslot, wz, attended, source_grad,
    load_sem, store_sem, zs, zr, xs, xr, ys, yr, qs, qr, us, ur, ts, tr, ps, pr, gs, gr, bs, br, cs, cr, es, er, fs, fr,
    ws, wr, vs, vr,
):
    a, c, x, y, z = here()
    d, g = a * 2 + c, x * 4 + y
    me = d * 8 + g
    pair = lax.div(z, 2)
    barrier = pltpu.get_barrier_semaphore()

    def along(o, n, at):
        return lax.rem(at + o + n, n)

    d_ahead = [along(k, 4, d) for k in range(4)]
    d_behind = [along(-k, 4, d) for k in range(4)]
    g_behind = [along(-k, 8, g) for k in range(8)]
    partners = [(k, dd) for k in range(8) for dd in range(4)][1:]

    def device(d_to, g_to):
        return {
            "dp_0": lax.div(d_to, 2), "dp_1": lax.rem(d_to, 2), "mp_0": lax.div(g_to, 4), "mp_1": lax.rem(g_to, 4),
        }

    def at_z(to):
        return {"mp_2": to}

    def at_y(to):
        return {"mp_1": to}

    other = 1 - x
    x_peer = {"mp_0": other}

    def rows(quarter):
        return pl.ds(pl.multiple_of(quarter * ROWS, ROWS), ROWS)

    loads = [
        pltpu.make_async_copy(sp.at[pl.ds(d * ROWS, ROWS)], spv, load_sem.at[0]),
        pltpu.make_async_copy(queries, qv, load_sem.at[1]),
        pltpu.make_async_copy(keys, kv, load_sem.at[2]),
        pltpu.make_async_copy(cotangent, cv, load_sem.at[3]),
        pltpu.make_async_copy(values, vv, load_sem.at[4]),
        pltpu.make_async_copy(kw, w.at[pl.ds(0, COLS)], load_sem.at[5]),
        pltpu.make_async_copy(vw, w.at[pl.ds(COLS, COLS)], load_sem.at[6]),
    ]
    loads[0].start()
    for o in reversed(RING):
        pl.semaphore_signal(barrier, inc=1, device_id=at_z(along(o, 8, z)), device_id_type=MESH)
    for k, dd in partners:
        pl.semaphore_signal(barrier, inc=1, device_id=device(d_ahead[dd], g_behind[k]), device_id_type=MESH)
    for load in loads[1:]:
        load.start()
    tt[me] = jnp.full((8, 128), tids[x * 32 + y * 8 + z], jnp.int32).astype(F32)
    tile = jnp.concatenate([soft(logits[...]).astype(BF16).astype(F32)] * ROWS, axis=0)
    row = lax.broadcasted_iota(jnp.int32, (128, 128), 0)
    loads[0].wait()
    total = jnp.zeros((COLS, 128), F32)
    for r in range(ROWS):
        weights = jnp.where(row // NTASK == r, tile, 0.0).astype(BF16)
        total += dot(spv[r], weights, NT)
    mix_t[x, y, z] = total.astype(BF16)
    pl.semaphore_wait(barrier, PLANE - 1 + 7)

    own = mix_t.at[x, y, z]
    push(own, own, xs, xr, x_peer).start()
    for o in RING:
        push(own, own, zs, zr.at[0, o], at_z(along(o, 8, z))).start()
    for k, dd in partners:
        push(tt.at[me], tt.at[me], ts, tr, device(d_ahead[dd], g_behind[k])).start()
    own = mix_t.at[other, y, z]
    push(own, own, xs, xr, x_peer).wait_recv()
    for o in RING:
        push(own, own, zs, zr.at[1, o], at_z(along(o, 8, z))).start()

    def pre(first, count):
        masked = lax.broadcasted_iota(jnp.int32, (SEQ, SEQ), 0) > lax.broadcasted_iota(jnp.int32, (SEQ, SEQ), 1)

        def step(n, carry):
            for e in range(PRE_HEADS):
                h = first + n * PRE_HEADS + e
                lanes = pl.ds(pl.multiple_of(h * DH, DH), DH)
                scores = dot(kv[:, lanes], qv[:, lanes], NT) * SCALE
                scores = jnp.where(masked, -1e30, scores)
                top = jnp.max(scores, axis=0, keepdims=True)
                exponent = jnp.exp(scores - top)
                grad = dot(vv[:, lanes], cv[:, lanes], NT)
                self_e[h] = exponent
                stat[h, 0:1] = top
                stat[h, 1:2] = jnp.sum(exponent, axis=0, keepdims=True)
                stat[h, 2:3] = jnp.sum(exponent * grad, axis=0, keepdims=True)
            return carry

        lax.fori_loop(0, count // PRE_HEADS, step, 0)

    for load in loads[1:5]:
        load.wait()
    up, down, across = along(1, 4, y), along(-1, 4, y), along(2, 4, y)
    halves = (x, other)

    def project(half, at):
        columns = pl.ds(pl.multiple_of(half * 2048 + at * 512, 512), 512)
        return dot(w[:, columns], mix_t[half, at].reshape(512, 128))

    def y_push(n, half, o):
        block = mix_t.at[half, y, along(-o, 8, z)]
        push(block, block, ys, yr.at[n, 0, o], at_y(up)).start()
        push(block, block, ys, yr.at[n, 1, o], at_y(down)).start()

    def y_relay(n, half, o, upward):
        source = along(-o, 8, z)
        from_down, from_up = mix_t.at[half, down, source], mix_t.at[half, up, source]
        push(from_down, from_down, ys, yr.at[n, 0, o], at_y(down)).wait_recv()
        if upward:
            push(from_down, from_down, qs, qr.at[n], at_y(up)).start()
        push(from_up, from_up, ys, yr.at[n, 1, o], at_y(up)).wait_recv()
        if not upward:
            push(from_up, from_up, qs, qr.at[n], at_y(down)).start()

    y_push(0, x, 0)
    y_push(1, other, 0)
    pre(0, 6)
    for n, half in enumerate(halves):
        for o in RING:
            block = mix_t.at[half, y, along(-o, 8, z)]
            push(block, block, zs, zr.at[n, o], at_z(along(-o, 8, z))).wait_recv()
            y_push(n, half, o)
        if n == 0:
            for place, o in enumerate((0, *RING[:4])):
                y_relay(0, x, o, place % 2 == 0)
            pre(6, 4)
    for load in loads[5:]:
        load.wait()
    for place, o in enumerate(RING[4:]):
        y_relay(0, x, o, (place + 5) % 2 == 0)
    total = project(x, y) + project(x, down) + project(x, up) + project(other, y)

    drain(tt.at[pl.ds(0, PLANE - 1)], tr)
    lane = lax.broadcasted_iota(jnp.int32, (ROWS, 128), 1)
    prompt_row = lax.broadcasted_iota(jnp.int32, (ROWS, 128), 0)
    lane_task = (lane % NTASK).astype(F32)
    lane_row = lane // NTASK == prompt_row

    def select(p, carry):
        task = jnp.concatenate([tt[p], tt[p]], axis=0)
        hit = jnp.where(lane_row & (task == lane_task), 1.0, 0.0)
        sel[rows(p), :] = hit.astype(BF16)
        return carry

    for place, o in enumerate((0, *RING)):
        y_relay(1, other, o, place % 2 == 0)
    lax.fori_loop(0, PLANE, select, 0)
    total += project(other, down) + project(other, up)
    for n, half in enumerate(halves):
        drain(mix_t.at[half, across], qr.at[n])
        total += project(half, across)

    tb[z] = total.astype(BF16)
    mate = pair * 2 + 1 - lax.rem(z, 2)

    def u_send(to):
        push(tb.at[z], tb.at[z], us, ur.at[along(to - z, 8, 0)], at_z(to)).start()

    def u_wait(source):
        push(tb.at[source], tb.at[source], us, ur.at[along(z - source, 8, 0)], at_z(source)).wait_recv()

    for hop in HOPS:
        to = along(-hop, 4, pair)
        for one in (mate,) if hop == 0 else (2 * to, 2 * to + 1):
            u_send(one)

    own_rows = rows(d)
    pieces = [along(hop, 4, pair) for hop in HOPS]
    for j, i in enumerate(pieces):
        if j == 0:
            pre(10, 12)
        for one in (mate,) if HOPS[j] == 0 else (2 * i, 2 * i + 1):
            u_wait(one)
        for which in range(2):
            part = slice(which * COLS, (which + 1) * COLS)
            table = jnp.concatenate([tb[2 * i, part, :], tb[2 * i + 1, part, :]], axis=0)
            out[i, :, which] = dot(sel[...], table, NT).astype(BF16).reshape(PLANE, ROWS, DH)
        for k, dd in partners:
            d_to, g_to = d_ahead[dd], g_behind[k]
            push(
                out.at[i, d_to * 8 + g_to], pp.at[i, g, :, own_rows, :], ps, pr.at[j, k], device(d_to, g_to)
            ).start()
        for which in range(2):
            pp[i, g, which, own_rows, :] = out[i, me, which]
    pre(22, 10)

    def head(i, g_here):
        h = g_here * 4 + i
        lanes = pl.ds(pl.multiple_of(h * DH, DH), DH)
        q, cot = qv[:, lanes], cv[:, lanes]
        scores = dot(pp[i, g_here, 0], q, NT) * SCALE
        grad = dot(pp[i, g_here, 1], cot, NT)
        self_top = stat[h, 0:1]
        top = jnp.maximum(jnp.max(scores, axis=0, keepdims=True), self_top)
        exponent = jnp.exp(scores - top)
        shrink = jnp.exp(self_top - top)
        inverse = 1.0 / (shrink * stat[h, 1:2] + jnp.sum(exponent, axis=0, keepdims=True))
        attention = exponent * inverse
        self_scale = shrink * inverse
        stat[h, 3:4] = self_scale
        rounded = attention.astype(BF16)
        pat[h] = rounded
        inner = self_scale * stat[h, 2:3] + jnp.sum(attention * grad, axis=0, keepdims=True)
        grad_scores = (attention * (grad - inner)).astype(BF16)
        gg[i, g_here, 0] = (dot(grad_scores, q) * SCALE).astype(BF16)
        gg[i, g_here, 1] = dot(rounded, cot).astype(BF16)

    def mid_step(j, i, ks, own_first):
        groups = [along(k, 8, g) for k in ks]
        for n, (k, g_here) in enumerate(zip(ks, groups)):
            if own_first and n == 0:
                drain(pp.at[i, g_here, :, pl.ds(0, PTOK - ROWS), :], pr.at[j, k])
            else:
                drain(pp.at[i, g_here], pr.at[j, k])
        for g_here in groups:
            head(i, g_here)
        for n, g_here in enumerate(groups):
            for dd in range(1 if own_first and n == 0 else 0, 4):
                d_to = d_ahead[dd]
                push(
                    gg.at[i, g_here, :, rows(d_to), :], rg.at[i, me], gs, gr.at[j], device(d_to, g_here)
                ).start()

    for j, i in enumerate(pieces):
        mid_step(j, i, list(range(MID_HEADS)), True)
        rg[i, me] = gg[i, g, :, own_rows, :]

        def later(n, carry, j=j, i=i):
            mid_step(j, i, [n * MID_HEADS + e for e in range(MID_HEADS)], False)
            return carry

        lax.fori_loop(1, 8 // MID_HEADS, later, 0)

    def post(first, count):
        def step(n, carry):
            for e in range(POST_HEADS):
                h = first + n * POST_HEADS + e
                lanes = pl.ds(pl.multiple_of(h * DH, DH), DH)
                self_part = (self_e[h] * stat[h, 3:4]).astype(BF16)
                prompt_values = pp[lax.rem(h, 4), lax.div(h, 4), 1]
                summed = dot(self_part, vv[:, lanes], TN) + dot(pat[h], prompt_values, TN)
                attended[:, lanes] = summed.astype(BF16)
            return carry

        lax.fori_loop(0, count // POST_HEADS, step, 0)
        lanes = pl.ds(first * DH, count * DH)
        store = pltpu.make_async_copy(attended.at[:, lanes], attended_hbm.at[:, lanes], store_sem.at[len(stores)])
        store.start()
        stores.append(store)

    stores = []

    post(0, 8)

    for j, i in enumerate(pieces):
        drain(rg.at[i, pl.ds(0, PLANE - 1)], gr.at[j])
        for which in range(2):
            summed = dot(rg[i, :, which].reshape(PLANE * ROWS, DH), sel[...], TN).astype(BF16)
            part = slice(which * COLS, (which + 1) * COLS)
            gz[2 * i, part, :] = summed[:COLS]
            gz[2 * i + 1, part, :] = summed[COLS:]
        for to in (mate,) if HOPS[j] == 0 else (2 * i, 2 * i + 1):
            push(gz.at[to], rz.at[along(to - z, 8, 0)], bs, br, at_z(to)).start()
    post(8, 8)
    grad = gz[z].astype(F32)
    drain(rz.at[pl.ds(1, 7)], br)
    for o in range(1, 8):
        grad += rz[o].astype(F32)
    grad_high = grad.astype(BF16)
    grad_low = (grad - grad_high.astype(F32)).astype(BF16)
    grad_both = jnp.concatenate([grad_high, grad_low], axis=1)

    def row_terms(half, at):
        columns = pl.ds(pl.multiple_of(half * 2048 + at * 512, 512), 512)
        terms = dot(w[:, columns], grad_both, TN)
        rt[half, at] = (terms[:, :128] + terms[:, 128:]).astype(BF16).reshape(8, COLS, 128)

    halves = (other, x)
    for n, half in enumerate(halves):
        for o in (2, 1, 3):
            to = along(o, 4, y)
            row_terms(half, to)
            push(rt.at[half, to], ry.at[n, o], cs, cr.at[n, o], at_y(to)).start()
        row_terms(half, y)

    def y_sum(n, half):
        four = rt[half, y].astype(F32)
        for o in (1, 3, 2):
            push(rt.at[half, y], ry.at[n, o], cs, cr.at[n, o], at_y(along(-o, 4, y))).wait_recv()
            four += ry[n, o].astype(F32)
        t2[n] = four.astype(BF16)
        for o in reversed(RING):
            to = along(o, 8, z)
            push(t2.at[n, to], rz2.at[n, o], es, er.at[n], at_z(to)).start()

    def z_sum(n):
        eight = t2[n, z].astype(F32)
        drain(rz2.at[n, pl.ds(1, 7)], er.at[n])
        for o in range(1, 8):
            eight += rz2[n, o].astype(F32)
        return eight

    post(16, 12)
    y_sum(0, other)
    y_sum(1, x)
    sx[...] = z_sum(0)
    push(sx, rx, fs, fr, x_peer).start()
    post(28, 4)
    mix = soft(logits[...])
    mine = z_sum(1)
    drain(rx, fr)
    mixture_grad = mine + rx[...]

    flipped = mixture_grad.T
    part = jnp.zeros((NTASK, NSRC), F32)
    for r in range(ROWS):
        part += jnp.dot(
            flipped[r * NTASK : (r + 1) * NTASK], spv[r].astype(F32), precision=HIGH, preferred_element_type=F32
        )
    wslot[me] = part

    for k, dd in partners:
        push(wslot.at[me], wslot.at[me], ws, wr, device(d_ahead[dd], g_behind[k])).start()
    tile = jnp.concatenate([mix] * ROWS, axis=0)
    lane = lax.broadcasted_iota(jnp.int32, (COLS, 128), 1)
    for r in range(ROWS):
        chosen = jnp.where(lane // NTASK == r, mixture_grad, 0.0)
        source_grad[r] = jnp.dot(chosen, tile, precision=HIGH, preferred_element_type=F32)
    store = pltpu.make_async_copy(source_grad, source_grad_hbm, store_sem.at[len(stores)])
    store.start()
    stores.append(store)
    drain(wslot.at[pl.ds(0, PLANE - 1)], wr)
    wz[z] = jnp.sum(wslot[...], axis=0)
    for o in reversed(RING):
        push(wz.at[z], wz.at[z], vs, vr, at_z(along(o, 8, z))).start()
    drain(mix_t.at[0, y, z], xs)
    drain(mix_t.at[:, y, pl.ds(0, 7)], zs)
    drain(mix_t.at[:, pl.ds(0, 2)], ys)
    drain(mix_t.at[:, y], qs)
    drain(tt.at[pl.ds(0, PLANE - 1)], ts)
    drain(tb.at[pl.ds(0, 7)], us)
    drain(out.at[:, pl.ds(0, PLANE - 1)], ps)
    drain(rg.at[:, pl.ds(0, PLANE - 1)], gs)
    drain(gz.at[pl.ds(0, 7)], bs)
    drain(rt.at[:, pl.ds(0, 3)], cs)
    drain(t2.at[:, pl.ds(0, 7)], es)
    drain(sx, fs)
    drain(wslot.at[pl.ds(0, PLANE - 1)], ws)
    for store in stores:
        store.wait()
    drain(wz.at[pl.ds(0, 7)], vr)
    weight_grad = jnp.sum(wz[...], axis=0)
    logits_grad[...] = mix * (weight_grad - jnp.sum(mix * weight_grad, axis=1, keepdims=True))
    drain(wz.at[pl.ds(0, 7)], vs)


PARTS = 4


def finish_kernel(attended_in, source_in, logits_in, attended_out, source_out, logits_out, held, tile, came, left):
    def parts(src, dst, sems):
        ends = ((src[0], dst[0], SEQ // PARTS), (src[1], dst[1], ROWS // PARTS))
        return [
            pltpu.make_async_copy(one.at[pl.ds(n * size, size)], to.at[pl.ds(n * size, size)], sems.at[k * PARTS + n])
            for k, (one, to, size) in enumerate(ends)
            for n in range(PARTS)
        ]

    arriving = parts((attended_in, source_in), (held, tile), came)
    leaving = parts((held, tile), (attended_out, source_out), left)
    for one in arriving:
        one.start()
    logits_out[...] = logits_in[...]
    for one, two in zip(arriving, leaving):
        one.wait()
        two.start()
    for two in leaving:
        two.wait()


def finish(attended, source_grad, logits_grad):
    any_space = pl.BlockSpec(memory_space=pl.ANY)
    vmem = pl.BlockSpec(memory_space=pltpu.VMEM)
    given = (attended, source_grad, logits_grad)
    return pl.pallas_call(
        finish_kernel,
        out_shape=tuple(jax.ShapeDtypeStruct(one.shape, one.dtype) for one in given),
        in_specs=[any_space, any_space, vmem],
        out_specs=(any_space, any_space, vmem),
        scratch_shapes=[
            pltpu.VMEM(attended.shape, BF16),
            pltpu.VMEM(source_grad.shape, F32),
            pltpu.SemaphoreType.DMA((2 * PARTS,)),
            pltpu.SemaphoreType.DMA((2 * PARTS,)),
        ],
        name="prompt_finish",
    )(*given)


def on_device(source_prompts, task_logits, task_ids, key_weight, value_weight, queries, keys, values, cotangent):
    any_space = pl.BlockSpec(memory_space=pl.ANY)
    vmem = pl.BlockSpec(memory_space=pltpu.VMEM)
    dma = pltpu.SemaphoreType.DMA
    block = (2, 8, COLS, 128)
    attended, source_grad, logits_grad = pl.pallas_call(
        kernel,
        out_shape=(
            jax.ShapeDtypeStruct((SEQ, D), BF16),
            jax.ShapeDtypeStruct((ROWS, COLS, NSRC), F32),
            jax.ShapeDtypeStruct((NTASK, NSRC), F32),
        ),
        in_specs=[pl.BlockSpec(memory_space=pltpu.SMEM), vmem] + [any_space] * 7,
        out_specs=(any_space, any_space, vmem),
        scratch_shapes=[
            pltpu.VMEM((ROWS, COLS, NSRC), BF16),
            pltpu.VMEM((2 * COLS, D), BF16),
            *[pltpu.VMEM((SEQ, D), BF16)] * 4,
            pltpu.VMEM((2, 4, 8, COLS, 128), BF16),
            pltpu.VMEM((8, 128, 128), BF16),
            pltpu.VMEM((PLANE, 8, 128), F32),
            pltpu.VMEM((PLANE * ROWS, 128), BF16),
            pltpu.VMEM((4, PLANE, 2, ROWS, DH), BF16),
            pltpu.VMEM((4, 8, 2, PTOK, DH), BF16),
            pltpu.VMEM((HEADS, 8, SEQ), F32),
            pltpu.VMEM((HEADS, SEQ, SEQ), F32),
            pltpu.VMEM((HEADS, PTOK, SEQ), BF16),
            pltpu.VMEM((4, 8, 2, PTOK, DH), BF16),
            pltpu.VMEM((4, PLANE, 2, ROWS, DH), BF16),
            pltpu.VMEM((8, 128, 128), BF16),
            pltpu.VMEM((8, 128, 128), BF16),
            pltpu.VMEM((2, 4, 8, COLS, 128), BF16),
            pltpu.VMEM((2, 4, 8, COLS, 128), BF16),
            pltpu.VMEM(block, BF16),
            pltpu.VMEM(block, BF16),
            pltpu.VMEM((COLS, 128), F32),
            pltpu.VMEM((COLS, 128), F32),
            pltpu.VMEM((PLANE, NTASK, NSRC), F32),
            pltpu.VMEM((8, NTASK, NSRC), F32),
            pltpu.VMEM((SEQ, D), BF16),
            pltpu.VMEM((ROWS, COLS, NSRC), F32),
            dma((7,)), dma((5,)), dma, dma((2, 8)), dma, dma, dma, dma((2, 2, 8)), dma, dma((2,)), dma, dma((8,)),
            dma, dma, dma, dma((4, 8)), dma, dma((4,)), dma, dma, dma, dma((2, 4)), dma, dma((2,)), dma, dma,
            dma, dma, dma, dma,
        ],
        compiler_params=pltpu.CompilerParams(collective_id=0, has_side_effects=True),
        name="prompt_step",
    )(
        task_ids, task_logits, source_prompts.transpose(1, 2, 0), key_weight.T, value_weight.T,
        queries[0], keys[0], values[0], cotangent[0],
    )
    attended, source_grad, logits_grad = finish(attended, source_grad, logits_grad)
    return attended[None], source_grad.transpose(2, 0, 1), logits_grad


def solution(mesh):
    torus = Mesh(mesh.devices.reshape(2, 2, 2, 4, 8), AXES)
    return jax.shard_map(
        on_device,
        mesh=torus,
        in_specs=(
            P(None, None, MP),
            P(),
            P(DP),
            P(None, MP),
            P(None, MP),
            P(AXES, None, None),
            P(AXES, None, None),
            P(AXES, None, None),
            P(AXES, None, None),
        ),
        out_specs=(P(AXES, None, None), P(None, DP, MP), P()),
        check_vma=False,
    )
```

```python
import jax
import jax.numpy as jnp
from jax import lax
from jax.experimental import pallas as pl
from jax.experimental.pallas import tpu as pltpu
from jax.sharding import Mesh
from jax.sharding import PartitionSpec as P

D = 4096
HEADS = 32
DH = 128
NSRC = 128
NTASK = 8
PTOK = 64
SEQ = 128
AXES = ("dp_0", "dp_1", "mp_0", "mp_1", "mp_2")
MP = ("mp_0", "mp_1", "mp_2")
DP = ("dp_0", "dp_1")
MESH = pl.DeviceIdType.MESH
ROWS = 16
COLS = 64
PLANE = 32
F32 = jnp.float32
BF16 = jnp.bfloat16
HIGH = lax.Precision.HIGHEST


def here():
    return tuple(lax.axis_index(name) for name in AXES)


def push(src, dst, sent, landed, device):
    return pltpu.make_async_remote_copy(
        src_ref=src, dst_ref=dst, send_sem=sent, recv_sem=landed, device_id=device, device_id_type=MESH
    )


def drain(ref, sem):
    pltpu.make_async_copy(ref, ref, sem).wait()


def far(partner):
    k, dd = partner
    return min(k % 4, 4 - k % 4) + (dd // 2) * 2 + k // 4


def soft(logits):
    exponent = jnp.exp(logits - jnp.max(logits, axis=1, keepdims=True))
    return exponent / jnp.sum(exponent, axis=1, keepdims=True)


NN = (((1,), (0,)), ((), ()))
NT = (((1,), (1,)), ((), ()))
TN = (((0,), (0,)), ((), ()))
SCALE = DH ** (-0.5)
HOPS = (0, 1, 3, 2)
MID = (1, 2, 3, 0)
RING = (1, 7, 2, 6, 3, 5, 4)
PRE_HEADS = 2
MID_HEADS = 2
POST_HEADS = 2


def dot(a, b, dims=NN):
    return lax.dot_general(a, b, dims, preferred_element_type=F32)


def kernel(
    tids, logits, sp, kw, vw, queries, keys, values, cotangent,
    attended, source_grad, logits_grad,
    spv, w, qv, kv, vv, cv, mix_t, tb, tt, sel, out, pp, stat, self_e, pat, gg, rg, gz, rz, rt, rl, ry, t2, rz2, sx, rx,
    wslot, wz,
    load_sem, zs, zr, xs, xr, ys, yr, qs, qr, us, ur, ts, tr, ps, pr, gs, gr, bs, br, cs, lr, cr, es, er, fs, fr,
    ws, wr, vs, vr,
):
    a, c, x, y, z = here()
    d, g = a * 2 + c, x * 4 + y
    me = d * 8 + g
    pair = lax.div(z, 2)
    barrier = pltpu.get_barrier_semaphore()

    def along(o, n, at):
        return lax.rem(at + o + n, n)

    d_ahead = [along(k, 4, d) for k in range(4)]
    d_behind = [along(-k, 4, d) for k in range(4)]
    g_behind = [along(-k, 8, g) for k in range(8)]
    partners = [(k, dd) for k in range(8) for dd in range(4)][1:]

    def device(d_to, g_to):
        return {
            "dp_0": lax.div(d_to, 2), "dp_1": lax.rem(d_to, 2), "mp_0": lax.div(g_to, 4), "mp_1": lax.rem(g_to, 4),
        }

    def at_z(to):
        return {"mp_2": to}

    def at_y(to):
        return {"mp_1": to}

    other = 1 - x
    x_peer = {"mp_0": other}

    def rows(quarter):
        return pl.ds(pl.multiple_of(quarter * ROWS, ROWS), ROWS)

    loads = [
        pltpu.make_async_copy(sp.at[pl.ds(d * ROWS, ROWS)], spv, load_sem.at[0]),
        pltpu.make_async_copy(queries, qv, load_sem.at[1]),
        pltpu.make_async_copy(keys, kv, load_sem.at[2]),
        pltpu.make_async_copy(cotangent, cv, load_sem.at[3]),
        pltpu.make_async_copy(values, vv, load_sem.at[4]),
        pltpu.make_async_copy(kw, w.at[pl.ds(0, COLS)], load_sem.at[5]),
        pltpu.make_async_copy(vw, w.at[pl.ds(COLS, COLS)], load_sem.at[6]),
    ]
    loads[0].start()
    for o in reversed(RING):
        pl.semaphore_signal(barrier, inc=1, device_id=at_z(along(o, 8, z)), device_id_type=MESH)
    for k, dd in sorted(partners, key=far, reverse=True):
        pl.semaphore_signal(barrier, inc=1, device_id=device(d_ahead[dd], g_behind[k]), device_id_type=MESH)
    for load in loads[1:]:
        load.start()
    tt[me] = jnp.full((8, 128), tids[x * 32 + y * 8 + z], jnp.int32).astype(F32)
    tile = jnp.concatenate([soft(logits[...]).astype(BF16).astype(F32)] * ROWS, axis=0)
    row = lax.broadcasted_iota(jnp.int32, (128, 128), 0)
    loads[0].wait()
    total = jnp.zeros((COLS, 128), F32)
    for r in range(ROWS):
        weights = jnp.where(row // NTASK == r, tile, 0.0).astype(BF16)
        total += dot(spv[r], weights, NT)
    mix_t[x, y, z] = total.astype(BF16)
    pl.semaphore_wait(barrier, PLANE - 1 + 7)

    own = mix_t.at[x, y, z]
    push(own, own, xs, xr, x_peer).start()
    for o in RING:
        push(own, own, zs, zr.at[0, o], at_z(along(o, 8, z))).start()
    for k, dd in partners:
        push(tt.at[me], tt.at[me], ts, tr, device(d_ahead[dd], g_behind[k])).start()
    own = mix_t.at[other, y, z]
    push(own, own, xs, xr, x_peer).wait_recv()
    for o in RING:
        push(own, own, zs, zr.at[1, o], at_z(along(o, 8, z))).start()

    def pre(first, count):
        masked = lax.broadcasted_iota(jnp.int32, (SEQ, SEQ), 0) > lax.broadcasted_iota(jnp.int32, (SEQ, SEQ), 1)

        def step(n, carry):
            for e in range(PRE_HEADS):
                h = first + n * PRE_HEADS + e
                lanes = pl.ds(pl.multiple_of(h * DH, DH), DH)
                scores = dot(kv[:, lanes], qv[:, lanes], NT) * SCALE
                scores = jnp.where(masked, -1e30, scores)
                top = jnp.max(scores, axis=0, keepdims=True)
                exponent = jnp.exp(scores - top)
                grad = dot(vv[:, lanes], cv[:, lanes], NT)
                self_e[h] = exponent
                stat[h, 0:1] = top
                stat[h, 1:2] = jnp.sum(exponent, axis=0, keepdims=True)
                stat[h, 2:3] = jnp.sum(exponent * grad, axis=0, keepdims=True)
            return carry

        lax.fori_loop(0, count // PRE_HEADS, step, 0)

    for load in loads[1:5]:
        load.wait()
    up, down, across = along(1, 4, y), along(-1, 4, y), along(2, 4, y)
    halves = (x, other)

    def project(half, at):
        columns = pl.ds(pl.multiple_of(half * 2048 + at * 512, 512), 512)
        return dot(w[:, columns], mix_t[half, at].reshape(512, 128))

    def y_push(n, half, o):
        block = mix_t.at[half, y, along(-o, 8, z)]
        push(block, block, ys, yr.at[n, 0, o], at_y(up)).start()
        push(block, block, ys, yr.at[n, 1, o], at_y(down)).start()

    def y_relay(n, half, o, upward):
        source = along(-o, 8, z)
        from_down, from_up = mix_t.at[half, down, source], mix_t.at[half, up, source]
        push(from_down, from_down, ys, yr.at[n, 0, o], at_y(down)).wait_recv()
        if upward:
            push(from_down, from_down, qs, qr.at[n], at_y(up)).start()
        push(from_up, from_up, ys, yr.at[n, 1, o], at_y(up)).wait_recv()
        if not upward:
            push(from_up, from_up, qs, qr.at[n], at_y(down)).start()

    y_push(0, x, 0)
    y_push(1, other, 0)
    pre(0, 6)
    for o in RING:
        for n, half in enumerate(halves):
            block = mix_t.at[half, y, along(-o, 8, z)]
            push(block, block, zs, zr.at[n, o], at_z(along(-o, 8, z))).wait_recv()
            y_push(n, half, o)
    places = tuple(enumerate((0, *RING)))
    for place, o in places[:6]:
        for n, half in enumerate(halves):
            y_relay(n, half, o, place % 2 == 0)
    for load in loads[5:]:
        load.wait()
    total = project(x, y) + project(other, y)
    for place, o in places[6:]:
        for n, half in enumerate(halves):
            y_relay(n, half, o, place % 2 == 0)
    total += project(x, down) + project(x, up) + project(other, down) + project(other, up)

    drain(tt.at[pl.ds(0, PLANE - 1)], tr)
    lane = lax.broadcasted_iota(jnp.int32, (ROWS, 128), 1)
    prompt_row = lax.broadcasted_iota(jnp.int32, (ROWS, 128), 0)
    lane_task = (lane % NTASK).astype(F32)
    lane_row = lane // NTASK == prompt_row

    def select(p, carry):
        task = jnp.concatenate([tt[p], tt[p]], axis=0)
        hit = jnp.where(lane_row & (task == lane_task), 1.0, 0.0)
        sel[rows(p), :] = hit.astype(BF16)
        return carry

    lax.fori_loop(0, PLANE, select, 0)
    for n, half in enumerate(halves):
        drain(mix_t.at[half, across], qr.at[n])
        total += project(half, across)

    tb[z] = total.astype(BF16)
    mate = pair * 2 + 1 - lax.rem(z, 2)

    def u_send(to):
        push(tb.at[z], tb.at[z], us, ur.at[along(to - z, 8, 0)], at_z(to)).start()

    def u_wait(source):
        push(tb.at[source], tb.at[source], us, ur.at[along(z - source, 8, 0)], at_z(source)).wait_recv()

    for hop in HOPS:
        to = along(-hop, 4, pair)
        for one in (mate,) if hop == 0 else (2 * to, 2 * to + 1):
            u_send(one)

    own_rows = rows(d)
    pieces = [along(hop, 4, pair) for hop in HOPS]
    for j, i in enumerate(pieces):
        if j == 0:
            pre(6, 12)
        for one in (mate,) if HOPS[j] == 0 else (2 * i, 2 * i + 1):
            u_wait(one)
        for which in range(2):
            part = slice(which * COLS, (which + 1) * COLS)
            table = jnp.concatenate([tb[2 * i, part, :], tb[2 * i + 1, part, :]], axis=0)
            out[i, :, which] = dot(sel[...], table, NT).astype(BF16).reshape(PLANE, ROWS, DH)
        for k, dd in partners:
            d_to, g_to = d_ahead[dd], g_behind[k]
            push(
                out.at[i, d_to * 8 + g_to], pp.at[i, g, :, own_rows, :], ps, pr.at[j, k], device(d_to, g_to)
            ).start()
        for which in range(2):
            pp[i, g, which, own_rows, :] = out[i, me, which]
    pre(18, 14)

    def head(i, g_here):
        h = g_here * 4 + i
        lanes = pl.ds(pl.multiple_of(h * DH, DH), DH)
        q, cot = qv[:, lanes], cv[:, lanes]
        scores = dot(pp[i, g_here, 0], q, NT) * SCALE
        grad = dot(pp[i, g_here, 1], cot, NT)
        self_top = stat[h, 0:1]
        top = jnp.maximum(jnp.max(scores, axis=0, keepdims=True), self_top)
        exponent = jnp.exp(scores - top)
        shrink = jnp.exp(self_top - top)
        inverse = 1.0 / (shrink * stat[h, 1:2] + jnp.sum(exponent, axis=0, keepdims=True))
        attention = exponent * inverse
        self_scale = shrink * inverse
        stat[h, 3:4] = self_scale
        rounded = attention.astype(BF16)
        pat[h] = rounded
        inner = self_scale * stat[h, 2:3] + jnp.sum(attention * grad, axis=0, keepdims=True)
        grad_scores = (attention * (grad - inner)).astype(BF16)
        gg[i, g_here, 0] = (dot(grad_scores, q) * SCALE).astype(BF16)
        gg[i, g_here, 1] = dot(rounded, cot).astype(BF16)

    def mid_step(j, i, ks, own_first):
        groups = [along(k, 8, g) for k in ks]
        for n, (k, g_here) in enumerate(zip(ks, groups)):
            if own_first and n == 0:
                drain(pp.at[i, g_here, :, pl.ds(0, PTOK - ROWS), :], pr.at[j, k])
            else:
                drain(pp.at[i, g_here], pr.at[j, k])
        for g_here in groups:
            head(i, g_here)
        for n, g_here in enumerate(groups):
            for dd in range(1 if own_first and n == 0 else 0, 4):
                d_to = d_ahead[dd]
                push(
                    gg.at[i, g_here, :, rows(d_to), :], rg.at[i, me], gs, gr.at[j], device(d_to, g_here)
                ).start()

    for j in MID:
        i = pieces[j]
        mid_step(j, i, list(range(MID_HEADS)), True)
        rg[i, me] = gg[i, g, :, own_rows, :]

        def later(n, carry, j=j, i=i):
            mid_step(j, i, [n * MID_HEADS + e for e in range(MID_HEADS)], False)
            return carry

        lax.fori_loop(1, 8 // MID_HEADS, later, 0)

    def post(first, count):
        def step(n, carry):
            for e in range(POST_HEADS):
                h = first + n * POST_HEADS + e
                lanes = pl.ds(pl.multiple_of(h * DH, DH), DH)
                self_part = (self_e[h] * stat[h, 3:4]).astype(BF16)
                prompt_values = pp[lax.rem(h, 4), lax.div(h, 4), 1]
                summed = dot(self_part, vv[:, lanes], TN) + dot(pat[h], prompt_values, TN)
                attended[:, lanes] = summed.astype(BF16)
            return carry

        lax.fori_loop(0, count // POST_HEADS, step, 0)

    post(0, 8)

    for j in MID:
        i = pieces[j]
        drain(rg.at[i, pl.ds(0, PLANE - 1)], gr.at[j])
        for which in range(2):
            summed = dot(rg[i, :, which].reshape(PLANE * ROWS, DH), sel[...], TN).astype(BF16)
            part = slice(which * COLS, (which + 1) * COLS)
            gz[2 * i, part, :] = summed[:COLS]
            gz[2 * i + 1, part, :] = summed[COLS:]
        for to in (mate,) if HOPS[j] == 0 else (2 * i, 2 * i + 1):
            push(gz.at[to], rz.at[along(to - z, 8, 0)], bs, br, at_z(to)).start()
    post(8, 8)
    grad = gz[z].astype(F32)
    drain(rz.at[pl.ds(1, 7)], br)
    for o in range(1, 8):
        grad += rz[o].astype(F32)
    grad_high = grad.astype(BF16)
    grad_low = (grad - grad_high.astype(F32)).astype(BF16)
    grad_both = jnp.concatenate([grad_high, grad_low], axis=1)

    def row_terms(half, at):
        columns = pl.ds(pl.multiple_of(half * 2048 + at * 512, 512), 512)
        terms = dot(w[:, columns], grad_both, TN)
        terms = (terms[:, :128] + terms[:, 128:]).astype(BF16).reshape(8, 2, COLS // 2, 128)
        for part in range(2):
            rt[half, part, at] = terms[:, part]

    def y_send(src, dst, landed, to):
        push(src, dst, cs, landed, at_y(to)).start()

    first, last = pl.ds(0, 4), pl.ds(4, 4)
    chunks = [(n, half, part) for n, half in enumerate((other, x)) for part in range(2)]
    for n, half in enumerate((other, x)):
        row_terms(half, across)
        for part in range(2):
            y_send(rt.at[half, part, across, first], rl.at[n, part, 0], lr.at[n, part, 0], up)
            y_send(rt.at[half, part, across, last], rl.at[n, part, 1], lr.at[n, part, 1], down)
        row_terms(half, up)
        for part in range(2):
            y_send(rt.at[half, part, up, last], ry.at[n, part, 0, last], cr.at[n, part, 0], up)
        row_terms(half, down)
        for part in range(2):
            y_send(rt.at[half, part, down, first], ry.at[n, part, 1, first], cr.at[n, part, 1], down)
    for half in (other, x):
        row_terms(half, y)

    def y_add(n, half, part):
        for way, to, piece in ((0, up, slice(0, 4)), (1, down, slice(4, 8))):
            drain(rl.at[n, part, way], lr.at[n, part, way])
            joined = rt[half, part, to, piece].astype(F32) + rl[n, part, way].astype(F32)
            rt[half, part, to, piece] = joined.astype(BF16)
            section = first if way == 0 else last
            y_send(rt.at[half, part, to, section], ry.at[n, part, way, section], cr.at[n, part, way], to)

    def y_sum(n, half, part):
        three = rt[half, part, y].astype(F32)
        for way in range(2):
            drain(ry.at[n, part, way], cr.at[n, part, way])
            three += ry[n, part, way].astype(F32)
        t2[n, part] = three.astype(BF16)
        for o in reversed(RING):
            to = along(o, 8, z)
            push(t2.at[n, part, to], rz2.at[n, part, o], es, er.at[n, part], at_z(to)).start()

    def z_sum(n, part):
        eight = t2[n, part, z].astype(F32)
        drain(rz2.at[n, part, pl.ds(1, 7)], er.at[n, part])
        for o in range(1, 8):
            eight += rz2[n, part, o].astype(F32)
        return eight

    y_add(*chunks[0])
    y_add(*chunks[1])
    post(16, 6)
    y_add(*chunks[2])
    y_add(*chunks[3])
    post(22, 10)
    for chunk in chunks:
        y_sum(*chunk)
    mix = soft(logits[...])
    for part in range(2):
        sx[part * 32 : (part + 1) * 32] = z_sum(0, part)
    push(sx, rx, fs, fr, x_peer).start()
    mine = jnp.concatenate([z_sum(1, 0), z_sum(1, 1)], axis=0)
    drain(rx, fr)
    mixture_grad = mine + rx[...]

    flipped = mixture_grad.T
    part = jnp.zeros((NTASK, NSRC), F32)
    for r in range(ROWS):
        part += jnp.dot(
            flipped[r * NTASK : (r + 1) * NTASK], spv[r].astype(F32), precision=HIGH, preferred_element_type=F32
        )
    wslot[me] = part

    for k, dd in partners:
        push(wslot.at[me], wslot.at[me], ws, wr, device(d_ahead[dd], g_behind[k])).start()
    tile = jnp.concatenate([mix] * ROWS, axis=0)
    lane = lax.broadcasted_iota(jnp.int32, (COLS, 128), 1)
    for r in range(ROWS):
        chosen = jnp.where(lane // NTASK == r, mixture_grad, 0.0)
        source_grad[r] = jnp.dot(chosen, tile, precision=HIGH, preferred_element_type=F32)
    drain(wslot.at[pl.ds(0, PLANE - 1)], wr)
    wz[z] = jnp.sum(wslot[...], axis=0)
    for o in reversed(RING):
        push(wz.at[z], wz.at[z], vs, vr, at_z(along(o, 8, z))).start()
    drain(mix_t.at[0, y, z], xs)
    drain(mix_t.at[:, y, pl.ds(0, 7)], zs)
    drain(mix_t.at[:, pl.ds(0, 2)], ys)
    drain(mix_t.at[:, y], qs)
    drain(tt.at[pl.ds(0, PLANE - 1)], ts)
    drain(tb.at[pl.ds(0, 7)], us)
    drain(out.at[:, pl.ds(0, PLANE - 1)], ps)
    drain(rg.at[:, pl.ds(0, PLANE - 1)], gs)
    drain(gz.at[pl.ds(0, 7)], bs)
    drain(rt.at[:, :, pl.ds(0, 3)], cs)
    drain(t2.at[:, :, pl.ds(0, 7)], es)
    drain(sx, fs)
    drain(wslot.at[pl.ds(0, PLANE - 1)], ws)
    drain(wz.at[pl.ds(0, 7)], vr)
    weight_grad = jnp.sum(wz[...], axis=0)
    logits_grad[...] = mix * (weight_grad - jnp.sum(mix * weight_grad, axis=1, keepdims=True))
    drain(wz.at[pl.ds(0, 7)], vs)


def on_device(source_prompts, task_logits, task_ids, key_weight, value_weight, queries, keys, values, cotangent):
    any_space = pl.BlockSpec(memory_space=pl.ANY)
    vmem = pl.BlockSpec(memory_space=pltpu.VMEM)
    dma = pltpu.SemaphoreType.DMA
    block = (8, COLS // 2, 128)
    attended, source_grad, logits_grad = pl.pallas_call(
        kernel,
        out_shape=(
            pltpu.VMEM((SEQ, D), BF16),
            pltpu.VMEM((ROWS, COLS, NSRC), F32),
            pltpu.VMEM((NTASK, NSRC), F32),
        ),
        in_specs=[pl.BlockSpec(memory_space=pltpu.SMEM), vmem] + [any_space] * 7,
        out_specs=(vmem, vmem, vmem),
        scratch_shapes=[
            pltpu.VMEM((ROWS, COLS, NSRC), BF16),
            pltpu.VMEM((2 * COLS, D), BF16),
            *[pltpu.VMEM((SEQ, D), BF16)] * 4,
            pltpu.VMEM((2, 4, 8, COLS, 128), BF16),
            pltpu.VMEM((8, 128, 128), BF16),
            pltpu.VMEM((PLANE, 8, 128), F32),
            pltpu.VMEM((PLANE * ROWS, 128), BF16),
            pltpu.VMEM((4, PLANE, 2, ROWS, DH), BF16),
            pltpu.VMEM((4, 8, 2, PTOK, DH), BF16),
            pltpu.VMEM((HEADS, 8, SEQ), F32),
            pltpu.VMEM((HEADS, SEQ, SEQ), F32),
            pltpu.VMEM((HEADS, PTOK, SEQ), BF16),
            pltpu.VMEM((4, 8, 2, PTOK, DH), BF16),
            pltpu.VMEM((4, PLANE, 2, ROWS, DH), BF16),
            pltpu.VMEM((8, 128, 128), BF16),
            pltpu.VMEM((8, 128, 128), BF16),
            pltpu.VMEM((2, 2, 4, *block), BF16),
            pltpu.VMEM((2, 2, 2, 4, COLS // 2, 128), BF16),
            pltpu.VMEM((2, 2, 2, *block), BF16),
            pltpu.VMEM((2, 2, *block), BF16),
            pltpu.VMEM((2, 2, *block), BF16),
            pltpu.VMEM((COLS, 128), F32),
            pltpu.VMEM((COLS, 128), F32),
            pltpu.VMEM((PLANE, NTASK, NSRC), F32),
            pltpu.VMEM((8, NTASK, NSRC), F32),
            dma((7,)), dma, dma((2, 8)), dma, dma, dma, dma((2, 2, 8)), dma, dma((2,)), dma, dma((8,)),
            dma, dma, dma, dma((4, 8)), dma, dma((4,)), dma, dma, dma, dma((2, 2, 2)), dma((2, 2, 2)), dma, dma((2, 2)), dma, dma,
            dma, dma, dma, dma,
        ],
        compiler_params=pltpu.CompilerParams(collective_id=0, has_side_effects=True),
        name="prompt_step",
    )(
        task_ids, task_logits, source_prompts.transpose(1, 2, 0), key_weight.T, value_weight.T,
        queries[0], keys[0], values[0], cotangent[0],
    )
    return attended[None], source_grad.transpose(2, 0, 1), logits_grad


def solution(mesh):
    torus = Mesh(mesh.devices.reshape(2, 2, 2, 4, 8), AXES)
    return jax.shard_map(
        on_device,
        mesh=torus,
        in_specs=(
            P(None, None, MP),
            P(),
            P(DP),
            P(None, MP),
            P(None, MP),
            P(AXES, None, None),
            P(AXES, None, None),
            P(AXES, None, None),
            P(AXES, None, None),
        ),
        out_specs=(P(AXES, None, None), P(None, DP, MP), P()),
        check_vma=False,
    )
```

```python
import jax
import jax.numpy as jnp
from jax import lax
from jax.experimental import pallas as pl
from jax.experimental.pallas import tpu as pltpu
from jax.sharding import Mesh
from jax.sharding import PartitionSpec as P

D = 4096
HEADS = 32
DH = 128
NSRC = 128
NTASK = 8
PTOK = 64
SEQ = 128
AXES = ("dp_0", "dp_1", "mp_0", "mp_1", "mp_2")
MP = ("mp_0", "mp_1", "mp_2")
DP = ("dp_0", "dp_1")
MESH = pl.DeviceIdType.MESH
ROWS = 16
COLS = 64
PLANE = 32
F32 = jnp.float32
BF16 = jnp.bfloat16
HIGH = lax.Precision.HIGHEST


def here():
    return tuple(lax.axis_index(name) for name in AXES)


def push(src, dst, sent, landed, device):
    return pltpu.make_async_remote_copy(
        src_ref=src, dst_ref=dst, send_sem=sent, recv_sem=landed, device_id=device, device_id_type=MESH
    )


def drain(ref, sem):
    pltpu.make_async_copy(ref, ref, sem).wait()


def far(partner):
    k, dd = partner
    return min(k % 4, 4 - k % 4) + (dd // 2) * 2 + k // 4


def soft(logits):
    exponent = jnp.exp(logits - jnp.max(logits, axis=1, keepdims=True))
    return exponent / jnp.sum(exponent, axis=1, keepdims=True)


NN = (((1,), (0,)), ((), ()))
NT = (((1,), (1,)), ((), ()))
TN = (((0,), (0,)), ((), ()))
SCALE = DH ** (-0.5)
HOPS = (0, 1, 3, 2)
MID = (1, 2, 3, 0)
RING = (1, 7, 2, 6, 3, 5, 4)
EARLY, LATE = (1, 7, 4, 3), (2, 6, 5)
PRE_HEADS = 2
MID_HEADS = 2
POST_HEADS = 2


def dot(a, b, dims=NN):
    return lax.dot_general(a, b, dims, preferred_element_type=F32)


def kernel(
    tids, logits, sp, kw, vw, queries, keys, values, cotangent,
    attended, source_grad, logits_grad,
    spv, w, wx, qv, kv, vv, cv, mix_t, tb, tt, sel, out, pp, stat, self_e, pat, gg, rg, gz, rz, gt, t2, rz2,
    wslot, wz,
    load_sem, zs, zr, xs, xr, ys, yr, qs, qr, us, ur, ts, tr, ps, pr, gs, gr, hs, hr, ks, kr, bs, br, cs, cr, es, er,
    ws, wr, vs, vr,
):
    a, c, x, y, z = here()
    d, g = a * 2 + c, x * 4 + y
    me = d * 8 + g
    pair = lax.div(z, 2)
    barrier = pltpu.get_barrier_semaphore()

    def along(o, n, at):
        return lax.rem(at + o + n, n)

    d_ahead = [along(k, 4, d) for k in range(4)]
    d_behind = [along(-k, 4, d) for k in range(4)]
    g_behind = [along(-k, 8, g) for k in range(8)]
    g_ahead = [along(k, 8, g) for k in range(8)]
    partners = [(k, dd) for k in range(8) for dd in range(4)][1:]

    def device(d_to, g_to):
        return {
            "dp_0": lax.div(d_to, 2), "dp_1": lax.rem(d_to, 2), "mp_0": lax.div(g_to, 4), "mp_1": lax.rem(g_to, 4),
        }

    def at_z(to):
        return {"mp_2": to}

    def at_g(to):
        return {"mp_0": lax.div(to, 4), "mp_1": lax.rem(to, 4)}

    def at_y(to):
        return {"mp_1": to}

    other = 1 - x
    x_peer = {"mp_0": other}

    def rows(quarter):
        return pl.ds(pl.multiple_of(quarter * ROWS, ROWS), ROWS)

    loads = [
        pltpu.make_async_copy(sp.at[pl.ds(d * ROWS, ROWS)], spv, load_sem.at[0]),
        pltpu.make_async_copy(queries, qv, load_sem.at[1]),
        pltpu.make_async_copy(keys, kv, load_sem.at[2]),
        pltpu.make_async_copy(cotangent, cv, load_sem.at[3]),
        pltpu.make_async_copy(values, vv, load_sem.at[4]),
        pltpu.make_async_copy(kw, w.at[pl.ds(0, COLS)], load_sem.at[5]),
        pltpu.make_async_copy(vw, w.at[pl.ds(COLS, COLS)], load_sem.at[6]),
    ]
    loads[0].start()
    for o in reversed(RING):
        pl.semaphore_signal(barrier, inc=1, device_id=at_z(along(o, 8, z)), device_id_type=MESH)
    for k, dd in sorted(partners, key=far, reverse=True):
        pl.semaphore_signal(barrier, inc=1, device_id=device(d_ahead[dd], g_behind[k]), device_id_type=MESH)
    for load in loads[1:]:
        load.start()
    tt[me] = jnp.full((8, 128), tids[x * 32 + y * 8 + z], jnp.int32).astype(F32)
    tile = jnp.concatenate([soft(logits[...]).astype(BF16).astype(F32)] * ROWS, axis=0)
    row = lax.broadcasted_iota(jnp.int32, (128, 128), 0)
    loads[0].wait()
    total = jnp.zeros((COLS, 128), F32)
    for r in range(ROWS):
        weights = jnp.where(row // NTASK == r, tile, 0.0).astype(BF16)
        total += dot(spv[r], weights, NT)
    mix_t[x, y, z] = total.astype(BF16)
    pl.semaphore_wait(barrier, PLANE - 1 + 7)

    own = mix_t.at[x, y, z]
    push(own, own, xs, xr, x_peer).start()
    for o in RING:
        push(own, own, zs, zr.at[0, o], at_z(along(o, 8, z))).start()
    for k, dd in partners:
        push(tt.at[me], tt.at[me], ts, tr, device(d_ahead[dd], g_behind[k])).start()
    own = mix_t.at[other, y, z]
    push(own, own, xs, xr, x_peer).wait_recv()
    for o in RING:
        push(own, own, zs, zr.at[1, o], at_z(along(o, 8, z))).start()

    def pre(first, count):
        masked = lax.broadcasted_iota(jnp.int32, (SEQ, SEQ), 0) > lax.broadcasted_iota(jnp.int32, (SEQ, SEQ), 1)

        def step(n, carry):
            for e in range(PRE_HEADS):
                h = first + n * PRE_HEADS + e
                lanes = pl.ds(pl.multiple_of(h * DH, DH), DH)
                scores = dot(kv[:, lanes], qv[:, lanes], NT) * SCALE
                scores = jnp.where(masked, -1e30, scores)
                top = jnp.max(scores, axis=0, keepdims=True)
                exponent = jnp.exp(scores - top)
                grad = dot(vv[:, lanes], cv[:, lanes], NT)
                self_e[h] = exponent
                stat[h, 0:1] = top
                stat[h, 1:2] = jnp.sum(exponent, axis=0, keepdims=True)
                stat[h, 2:3] = jnp.sum(exponent * grad, axis=0, keepdims=True)
            return carry

        lax.fori_loop(0, count // PRE_HEADS, step, 0)

    for load in loads[1:5]:
        load.wait()
    up, down, across = along(1, 4, y), along(-1, 4, y), along(2, 4, y)
    halves = (x, other)

    def project(half, at):
        columns = pl.ds(pl.multiple_of(half * 2048 + at * 512, 512), 512)
        return dot(w[:, columns], mix_t[half, at].reshape(512, 128))

    def y_push(n, half, o):
        block = mix_t.at[half, y, along(-o, 8, z)]
        push(block, block, ys, yr.at[n, 0, o], at_y(up)).start()
        push(block, block, ys, yr.at[n, 1, o], at_y(down)).start()

    def y_relay(n, half, o, upward):
        source = along(-o, 8, z)
        from_down, from_up = mix_t.at[half, down, source], mix_t.at[half, up, source]
        push(from_down, from_down, ys, yr.at[n, 0, o], at_y(down)).wait_recv()
        if upward:
            push(from_down, from_down, qs, qr.at[n], at_y(up)).start()
        push(from_up, from_up, ys, yr.at[n, 1, o], at_y(up)).wait_recv()
        if not upward:
            push(from_up, from_up, qs, qr.at[n], at_y(down)).start()

    y_push(0, x, 0)
    y_push(1, other, 0)
    pre(0, 6)
    for o in RING:
        for n, half in enumerate(halves):
            block = mix_t.at[half, y, along(-o, 8, z)]
            push(block, block, zs, zr.at[n, o], at_z(along(-o, 8, z))).wait_recv()
            y_push(n, half, o)
    places = tuple(enumerate((0, *RING)))
    for place, o in places[:6]:
        for n, half in enumerate(halves):
            y_relay(n, half, o, place % 2 == 0)
    for load in loads[5:]:
        load.wait()
    total = project(x, y) + project(other, y)
    for place, o in places[6:]:
        for n, half in enumerate(halves):
            y_relay(n, half, o, place % 2 == 0)
    total += project(x, down) + project(x, up) + project(other, down) + project(other, up)

    drain(tt.at[pl.ds(0, PLANE - 1)], tr)
    lane = lax.broadcasted_iota(jnp.int32, (ROWS, 128), 1)
    prompt_row = lax.broadcasted_iota(jnp.int32, (ROWS, 128), 0)
    lane_task = (lane % NTASK).astype(F32)
    lane_row = lane // NTASK == prompt_row

    def select(p, carry):
        task = jnp.concatenate([tt[p], tt[p]], axis=0)
        hit = jnp.where(lane_row & (task == lane_task), 1.0, 0.0)
        sel[rows(p), :] = hit.astype(BF16)
        return carry

    lax.fori_loop(0, PLANE, select, 0)
    for n, half in enumerate(halves):
        drain(mix_t.at[half, across], qr.at[n])
        total += project(half, across)

    tb[z] = total.astype(BF16)
    mate = pair * 2 + 1 - lax.rem(z, 2)

    def u_send(to):
        push(tb.at[z], tb.at[z], us, ur.at[along(to - z, 8, 0)], at_z(to)).start()

    def u_wait(source):
        push(tb.at[source], tb.at[source], us, ur.at[along(z - source, 8, 0)], at_z(source)).wait_recv()

    for hop in HOPS:
        to = along(-hop, 4, pair)
        for one in (mate,) if hop == 0 else (2 * to, 2 * to + 1):
            u_send(one)

    half = pl.ds(pl.multiple_of(c * COLS, COLS), COLS)
    missing = pl.ds(pl.multiple_of((1 - c) * COLS, COLS), COLS)

    def features(at):
        return pl.ds(pl.multiple_of(at * 512, 512), 512)

    def fetch(k):
        to = g_behind[k]
        push(w.at[half, features(to)], wx.at[g, half], hs, hr.at[k], at_g(to)).start()

    def hand_over(k):
        block = wx.at[g_ahead[k], half]
        push(block, block, hs, hr.at[k], at_g(g_ahead[k])).wait_recv()
        push(block, block, ks, kr.at[k], {"dp_1": 1 - c}).start()

    for k in EARLY:
        fetch(k)

    own_rows = rows(d)
    pieces = [along(hop, 4, pair) for hop in HOPS]
    for j, i in enumerate(pieces):
        if j == 0:
            pre(6, 12)
        for one in (mate,) if HOPS[j] == 0 else (2 * i, 2 * i + 1):
            u_wait(one)
        for which in range(2):
            part = slice(which * COLS, (which + 1) * COLS)
            table = jnp.concatenate([tb[2 * i, part, :], tb[2 * i + 1, part, :]], axis=0)
            out[i, :, which] = dot(sel[...], table, NT).astype(BF16).reshape(PLANE, ROWS, DH)
        for k, dd in partners:
            d_to, g_to = d_ahead[dd], g_behind[k]
            push(
                out.at[i, d_to * 8 + g_to], pp.at[i, g, :, own_rows, :], ps, pr.at[j, k], device(d_to, g_to)
            ).start()
        for which in range(2):
            pp[i, g, which, own_rows, :] = out[i, me, which]
    pre(18, 14)
    for k in EARLY:
        hand_over(k)

    def head(i, g_here):
        h = g_here * 4 + i
        lanes = pl.ds(pl.multiple_of(h * DH, DH), DH)
        q, cot = qv[:, lanes], cv[:, lanes]
        scores = dot(pp[i, g_here, 0], q, NT) * SCALE
        grad = dot(pp[i, g_here, 1], cot, NT)
        self_top = stat[h, 0:1]
        top = jnp.maximum(jnp.max(scores, axis=0, keepdims=True), self_top)
        exponent = jnp.exp(scores - top)
        shrink = jnp.exp(self_top - top)
        inverse = 1.0 / (shrink * stat[h, 1:2] + jnp.sum(exponent, axis=0, keepdims=True))
        attention = exponent * inverse
        self_scale = shrink * inverse
        stat[h, 3:4] = self_scale
        rounded = attention.astype(BF16)
        pat[h] = rounded
        inner = self_scale * stat[h, 2:3] + jnp.sum(attention * grad, axis=0, keepdims=True)
        grad_scores = (attention * (grad - inner)).astype(BF16)
        gg[i, g_here, 0] = (dot(grad_scores, q) * SCALE).astype(BF16)
        gg[i, g_here, 1] = dot(rounded, cot).astype(BF16)

    def mid_step(j, i, ks, own_first):
        groups = [along(k, 8, g) for k in ks]
        for n, (k, g_here) in enumerate(zip(ks, groups)):
            if own_first and n == 0:
                drain(pp.at[i, g_here, :, pl.ds(0, PTOK - ROWS), :], pr.at[j, k])
            else:
                drain(pp.at[i, g_here], pr.at[j, k])
        for g_here in groups:
            head(i, g_here)
        for n, g_here in enumerate(groups):
            for dd in range(1 if own_first and n == 0 else 0, 4):
                d_to = d_ahead[dd]
                push(
                    gg.at[i, g_here, :, rows(d_to), :], rg.at[i, me], gs, gr.at[j], device(d_to, g_here)
                ).start()

    for j in MID:
        i = pieces[j]
        mid_step(j, i, list(range(MID_HEADS)), True)
        rg[i, me] = gg[i, g, :, own_rows, :]

        def later(n, carry, j=j, i=i):
            mid_step(j, i, [n * MID_HEADS + e for e in range(MID_HEADS)], False)
            return carry

        lax.fori_loop(1, 8 // MID_HEADS, later, 0)

    def post(first, count):
        def step(n, carry):
            for e in range(POST_HEADS):
                h = first + n * POST_HEADS + e
                lanes = pl.ds(pl.multiple_of(h * DH, DH), DH)
                self_part = (self_e[h] * stat[h, 3:4]).astype(BF16)
                prompt_values = pp[lax.rem(h, 4), lax.div(h, 4), 1]
                summed = dot(self_part, vv[:, lanes], TN) + dot(pat[h], prompt_values, TN)
                attended[:, lanes] = summed.astype(BF16)
            return carry

        lax.fori_loop(0, count // POST_HEADS, step, 0)

    for k in LATE:
        fetch(k)
    post(0, 8)

    for j in MID:
        i = pieces[j]
        drain(rg.at[i, pl.ds(0, PLANE - 1)], gr.at[j])
        for which in range(2):
            summed = dot(rg[i, :, which].reshape(PLANE * ROWS, DH), sel[...], TN).astype(BF16)
            part = slice(which * COLS, (which + 1) * COLS)
            gz[2 * i, part, :] = summed[:COLS]
            gz[2 * i + 1, part, :] = summed[COLS:]
        for to in (mate,) if HOPS[j] == 0 else (2 * i, 2 * i + 1):
            push(gz.at[to], rz.at[along(to - z, 8, 0)], bs, br, at_z(to)).start()
    for k in LATE:
        hand_over(k)
    post(8, 8)
    grad = gz[z].astype(F32)
    drain(rz.at[pl.ds(1, 7)], br)
    for o in range(1, 8):
        grad += rz[o].astype(F32)
    gt[g] = grad.astype(BF16)

    for k in range(1, 8):
        push(gt.at[g], gt.at[g], cs, cr.at[k], at_g(g_behind[k])).start()
    post(16, 10)
    terms = dot(w[:, features(g)], gt[g], TN)
    for k in range(1, 8):
        source = g_ahead[k]
        block = wx.at[source, missing]
        push(block, block, ks, kr.at[k], {"dp_1": 1 - c}).wait_recv()
        push(gt.at[source], gt.at[source], cs, cr.at[k], at_g(source)).wait_recv()
        terms += dot(wx[source], gt[source], TN)
    t2[...] = terms.astype(BF16).reshape(8, COLS, 128)
    for o in reversed(RING):
        to = along(o, 8, z)
        push(t2.at[to], rz2.at[o], es, er, at_z(to)).start()
    post(26, 6)
    mix = soft(logits[...])
    mixture_grad = t2[z].astype(F32)
    drain(rz2.at[pl.ds(1, 7)], er)
    for o in range(1, 8):
        mixture_grad += rz2[o].astype(F32)

    flipped = mixture_grad.T
    part = jnp.zeros((NTASK, NSRC), F32)
    for r in range(ROWS):
        part += jnp.dot(
            flipped[r * NTASK : (r + 1) * NTASK], spv[r].astype(F32), precision=HIGH, preferred_element_type=F32
        )
    wslot[me] = part

    for k, dd in partners:
        push(wslot.at[me], wslot.at[me], ws, wr, device(d_ahead[dd], g_behind[k])).start()
    tile = jnp.concatenate([mix] * ROWS, axis=0)
    lane = lax.broadcasted_iota(jnp.int32, (COLS, 128), 1)
    for r in range(ROWS):
        chosen = jnp.where(lane // NTASK == r, mixture_grad, 0.0)
        source_grad[r] = jnp.dot(chosen, tile, precision=HIGH, preferred_element_type=F32)
    drain(wslot.at[pl.ds(0, PLANE - 1)], wr)
    wz[z] = jnp.sum(wslot[...], axis=0)
    for o in reversed(RING):
        push(wz.at[z], wz.at[z], vs, vr, at_z(along(o, 8, z))).start()
    drain(mix_t.at[0, y, z], xs)
    drain(mix_t.at[:, y, pl.ds(0, 7)], zs)
    drain(mix_t.at[:, pl.ds(0, 2)], ys)
    drain(mix_t.at[:, y], qs)
    drain(tt.at[pl.ds(0, PLANE - 1)], ts)
    drain(tb.at[pl.ds(0, 7)], us)
    drain(out.at[:, pl.ds(0, PLANE - 1)], ps)
    drain(rg.at[:, pl.ds(0, PLANE - 1)], gs)
    drain(gz.at[pl.ds(0, 7)], bs)
    drain(wx.at[pl.ds(0, 7), half], hs)
    drain(wx.at[pl.ds(0, 7), half], ks)
    drain(gt.at[pl.ds(0, 7)], cs)
    drain(t2.at[pl.ds(0, 7)], es)
    drain(wslot.at[pl.ds(0, PLANE - 1)], ws)
    drain(wz.at[pl.ds(0, 7)], vr)
    weight_grad = jnp.sum(wz[...], axis=0)
    logits_grad[...] = mix * (weight_grad - jnp.sum(mix * weight_grad, axis=1, keepdims=True))
    drain(wz.at[pl.ds(0, 7)], vs)


def on_device(source_prompts, task_logits, task_ids, key_weight, value_weight, queries, keys, values, cotangent):
    any_space = pl.BlockSpec(memory_space=pl.ANY)
    vmem = pl.BlockSpec(memory_space=pltpu.VMEM)
    dma = pltpu.SemaphoreType.DMA
    attended, source_grad, logits_grad = pl.pallas_call(
        kernel,
        out_shape=(
            pltpu.VMEM((SEQ, D), BF16),
            pltpu.VMEM((ROWS, COLS, NSRC), F32),
            pltpu.VMEM((NTASK, NSRC), F32),
        ),
        in_specs=[pl.BlockSpec(memory_space=pltpu.SMEM), vmem] + [any_space] * 7,
        out_specs=(vmem, vmem, vmem),
        scratch_shapes=[
            pltpu.VMEM((ROWS, COLS, NSRC), BF16),
            pltpu.VMEM((2 * COLS, D), BF16),
            pltpu.VMEM((8, 2 * COLS, 512), BF16),
            *[pltpu.VMEM((SEQ, D), BF16)] * 4,
            pltpu.VMEM((2, 4, 8, COLS, 128), BF16),
            pltpu.VMEM((8, 128, 128), BF16),
            pltpu.VMEM((PLANE, 8, 128), F32),
            pltpu.VMEM((PLANE * ROWS, 128), BF16),
            pltpu.VMEM((4, PLANE, 2, ROWS, DH), BF16),
            pltpu.VMEM((4, 8, 2, PTOK, DH), BF16),
            pltpu.VMEM((HEADS, 8, SEQ), F32),
            pltpu.VMEM((HEADS, SEQ, SEQ), F32),
            pltpu.VMEM((HEADS, PTOK, SEQ), BF16),
            pltpu.VMEM((4, 8, 2, PTOK, DH), BF16),
            pltpu.VMEM((4, PLANE, 2, ROWS, DH), BF16),
            pltpu.VMEM((8, 128, 128), BF16),
            pltpu.VMEM((8, 128, 128), BF16),
            pltpu.VMEM((8, 128, 128), BF16),
            pltpu.VMEM((8, COLS, 128), BF16),
            pltpu.VMEM((8, COLS, 128), BF16),
            pltpu.VMEM((PLANE, NTASK, NSRC), F32),
            pltpu.VMEM((8, NTASK, NSRC), F32),
            dma((7,)), dma, dma((2, 8)), dma, dma, dma, dma((2, 2, 8)), dma, dma((2,)), dma, dma((8,)),
            dma, dma, dma, dma((4, 8)), dma, dma((4,)), dma, dma((8,)), dma, dma((8,)),
            dma, dma, dma, dma((8,)), dma, dma,
            dma, dma, dma, dma,
        ],
        compiler_params=pltpu.CompilerParams(collective_id=0, has_side_effects=True),
        name="prompt_step",
    )(
        task_ids, task_logits, source_prompts.transpose(1, 2, 0), key_weight.T, value_weight.T,
        queries[0], keys[0], values[0], cotangent[0],
    )
    return attended[None], source_grad.transpose(2, 0, 1), logits_grad


def solution(mesh):
    torus = Mesh(mesh.devices.reshape(2, 2, 2, 4, 8), AXES)
    return jax.shard_map(
        on_device,
        mesh=torus,
        in_specs=(
            P(None, None, MP),
            P(),
            P(DP),
            P(None, MP),
            P(None, MP),
            P(AXES, None, None),
            P(AXES, None, None),
            P(AXES, None, None),
            P(AXES, None, None),
        ),
        out_specs=(P(AXES, None, None), P(None, DP, MP), P()),
        check_vma=False,
    )
```

```python
import jax
import jax.numpy as jnp
from jax import lax
from jax.experimental import pallas as pl
from jax.experimental.pallas import tpu as pltpu
from jax.sharding import Mesh
from jax.sharding import PartitionSpec as P

D = 4096
HEADS = 32
DH = 128
NSRC = 128
NTASK = 8
PTOK = 64
SEQ = 128
AXES = ("dp_0", "dp_1", "mp_0", "mp_1", "mp_2")
MP = ("mp_0", "mp_1", "mp_2")
DP = ("dp_0", "dp_1")
MESH = pl.DeviceIdType.MESH
ROWS = 16
COLS = 64
PLANE = 32
F32 = jnp.float32
BF16 = jnp.bfloat16
HIGH = lax.Precision.HIGHEST


def here():
    return tuple(lax.axis_index(name) for name in AXES)


def push(src, dst, sent, landed, device):
    return pltpu.make_async_remote_copy(
        src_ref=src, dst_ref=dst, send_sem=sent, recv_sem=landed, device_id=device, device_id_type=MESH
    )


def drain(ref, sem):
    pltpu.make_async_copy(ref, ref, sem).wait()


def far(partner):
    k, dd = partner
    return min(k % 4, 4 - k % 4) + (dd // 2) * 2 + k // 4


def soft(logits):
    exponent = jnp.exp(logits - jnp.max(logits, axis=1, keepdims=True))
    return exponent / jnp.sum(exponent, axis=1, keepdims=True)


NN = (((1,), (0,)), ((), ()))
NT = (((1,), (1,)), ((), ()))
TN = (((0,), (0,)), ((), ()))
SCALE = DH ** (-0.5)
HOPS = (0, 1, 3, 2)
MID = (1, 2, 3, 0)
RING = (1, 7, 2, 6, 3, 5, 4)
NEAR = (4, 1, 7, 3, 5, 2, 6)
EARLY, LATE = (1, 7, 4, 3), (2, 6, 5)
PRE_HEADS = 2
MID_HEADS = 2
POST_HEADS = 2


def dot(a, b, dims=NN):
    return lax.dot_general(a, b, dims, preferred_element_type=F32)


def kernel(
    tids, logits, sp, kw, vw, queries, keys, values, cotangent,
    attended, source_grad, logits_grad,
    spv, w, wx, qv, kv, vv, cv, mix_t, tb, tt, sel, out, pp, stat, self_e, pat, gg, rg, gz, rz, gt, t2, rz2,
    wslot, wz,
    load_sem, zs, zr, xs, xr, ys, yr, qs, qr, us, ur, ts, tr, ps, pr, gs, gr, hs, hr, ks, kr, bs, br, cs, cr, es, er,
    ws, wr, vs, vr,
):
    a, c, x, y, z = here()
    d, g = a * 2 + c, x * 4 + y
    me = d * 8 + g
    pair = lax.div(z, 2)
    barrier = pltpu.get_barrier_semaphore()

    def along(o, n, at):
        return lax.rem(at + o + n, n)

    d_ahead = [along(k, 4, d) for k in range(4)]
    d_behind = [along(-k, 4, d) for k in range(4)]
    g_behind = [along(-k, 8, g) for k in range(8)]
    g_ahead = [along(k, 8, g) for k in range(8)]
    partners = [(k, dd) for k in range(8) for dd in range(4)][1:]

    def device(d_to, g_to):
        return {
            "dp_0": lax.div(d_to, 2), "dp_1": lax.rem(d_to, 2), "mp_0": lax.div(g_to, 4), "mp_1": lax.rem(g_to, 4),
        }

    def at_z(to):
        return {"mp_2": to}

    def at_g(to):
        return {"mp_0": lax.div(to, 4), "mp_1": lax.rem(to, 4)}

    def at_y(to):
        return {"mp_1": to}

    other = 1 - x
    x_peer = {"mp_0": other}

    def rows(quarter):
        return pl.ds(pl.multiple_of(quarter * ROWS, ROWS), ROWS)

    loads = [
        pltpu.make_async_copy(sp.at[pl.ds(d * ROWS, ROWS)], spv, load_sem.at[0]),
        pltpu.make_async_copy(queries, qv, load_sem.at[1]),
        pltpu.make_async_copy(keys, kv, load_sem.at[2]),
        pltpu.make_async_copy(cotangent, cv, load_sem.at[3]),
        pltpu.make_async_copy(values, vv, load_sem.at[4]),
        pltpu.make_async_copy(kw, w.at[pl.ds(0, COLS)], load_sem.at[5]),
        pltpu.make_async_copy(vw, w.at[pl.ds(COLS, COLS)], load_sem.at[6]),
    ]
    loads[0].start()
    for o in reversed(RING):
        pl.semaphore_signal(barrier, inc=1, device_id=at_z(along(o, 8, z)), device_id_type=MESH)
    for k, dd in sorted(partners, key=far, reverse=True):
        pl.semaphore_signal(barrier, inc=1, device_id=device(d_ahead[dd], g_behind[k]), device_id_type=MESH)
    for load in loads[1:]:
        load.start()
    tt[me] = jnp.full((8, 128), tids[x * 32 + y * 8 + z], jnp.int32).astype(F32)
    tile = jnp.concatenate([soft(logits[...]).astype(BF16).astype(F32)] * ROWS, axis=0)
    row = lax.broadcasted_iota(jnp.int32, (128, 128), 0)
    loads[0].wait()
    total = jnp.zeros((COLS, 128), F32)
    for r in range(ROWS):
        weights = jnp.where(row // NTASK == r, tile, 0.0).astype(BF16)
        total += dot(spv[r], weights, NT)
    mix_t[x, y, z] = total.astype(BF16)
    pl.semaphore_wait(barrier, PLANE - 1 + 7)

    own = mix_t.at[x, y, z]
    push(own, own, xs, xr, x_peer).start()
    for o in RING:
        push(own, own, zs, zr.at[0, o], at_z(along(o, 8, z))).start()
    for k, dd in partners:
        push(tt.at[me], tt.at[me], ts, tr, device(d_ahead[dd], g_behind[k])).start()
    own = mix_t.at[other, y, z]
    push(own, own, xs, xr, x_peer).wait_recv()
    for o in RING:
        push(own, own, zs, zr.at[1, o], at_z(along(o, 8, z))).start()

    def pre(first, count):
        masked = lax.broadcasted_iota(jnp.int32, (SEQ, SEQ), 0) > lax.broadcasted_iota(jnp.int32, (SEQ, SEQ), 1)

        def step(n, carry):
            for e in range(PRE_HEADS):
                h = first + n * PRE_HEADS + e
                lanes = pl.ds(pl.multiple_of(h * DH, DH), DH)
                scores = dot(kv[:, lanes], qv[:, lanes], NT) * SCALE
                scores = jnp.where(masked, -1e30, scores)
                top = jnp.max(scores, axis=0, keepdims=True)
                exponent = jnp.exp(scores - top)
                grad = dot(vv[:, lanes], cv[:, lanes], NT)
                self_e[h] = exponent
                stat[h, 0:1] = top
                stat[h, 1:2] = jnp.sum(exponent, axis=0, keepdims=True)
                stat[h, 2:3] = jnp.sum(exponent * grad, axis=0, keepdims=True)
            return carry

        lax.fori_loop(0, count // PRE_HEADS, step, 0)

    for load in loads[1:5]:
        load.wait()
    up, down, across = along(1, 4, y), along(-1, 4, y), along(2, 4, y)
    halves = (x, other)

    def project(half, at):
        columns = pl.ds(pl.multiple_of(half * 2048 + at * 512, 512), 512)
        return dot(w[:, columns], mix_t[half, at].reshape(512, 128))

    def y_push(n, half, o):
        block = mix_t.at[half, y, along(-o, 8, z)]
        push(block, block, ys, yr.at[n, 0, o], at_y(up)).start()
        push(block, block, ys, yr.at[n, 1, o], at_y(down)).start()

    def y_relay(n, half, o, upward):
        source = along(-o, 8, z)
        from_down, from_up = mix_t.at[half, down, source], mix_t.at[half, up, source]
        push(from_down, from_down, ys, yr.at[n, 0, o], at_y(down)).wait_recv()
        if upward:
            push(from_down, from_down, qs, qr.at[n], at_y(up)).start()
        push(from_up, from_up, ys, yr.at[n, 1, o], at_y(up)).wait_recv()
        if not upward:
            push(from_up, from_up, qs, qr.at[n], at_y(down)).start()

    y_push(0, x, 0)
    y_push(1, other, 0)
    pre(0, 6)
    for o in RING:
        for n, half in enumerate(halves):
            block = mix_t.at[half, y, along(-o, 8, z)]
            push(block, block, zs, zr.at[n, o], at_z(along(-o, 8, z))).wait_recv()
            y_push(n, half, o)
    places = tuple(enumerate((0, *RING)))
    for place, o in places[:6]:
        for n, half in enumerate(halves):
            y_relay(n, half, o, place % 2 == 0)
    for load in loads[5:]:
        load.wait()
    total = project(x, y) + project(other, y)
    for place, o in places[6:]:
        for n, half in enumerate(halves):
            y_relay(n, half, o, place % 2 == 0)
    total += project(x, down) + project(x, up) + project(other, down) + project(other, up)

    drain(tt.at[pl.ds(0, PLANE - 1)], tr)
    lane = lax.broadcasted_iota(jnp.int32, (ROWS, 128), 1)
    prompt_row = lax.broadcasted_iota(jnp.int32, (ROWS, 128), 0)
    lane_task = (lane % NTASK).astype(F32)
    lane_row = lane // NTASK == prompt_row

    def select(p, carry):
        task = jnp.concatenate([tt[p], tt[p]], axis=0)
        hit = jnp.where(lane_row & (task == lane_task), 1.0, 0.0)
        sel[rows(p), :] = hit.astype(BF16)
        return carry

    lax.fori_loop(0, PLANE, select, 0)
    for n, half in enumerate(halves):
        drain(mix_t.at[half, across], qr.at[n])
        total += project(half, across)

    tb[z] = total.astype(BF16)
    mate = pair * 2 + 1 - lax.rem(z, 2)

    def u_send(to):
        push(tb.at[z], tb.at[z], us, ur.at[along(to - z, 8, 0)], at_z(to)).start()

    def u_wait(source):
        push(tb.at[source], tb.at[source], us, ur.at[along(z - source, 8, 0)], at_z(source)).wait_recv()

    for hop in HOPS:
        to = along(-hop, 4, pair)
        for one in (mate,) if hop == 0 else (2 * to, 2 * to + 1):
            u_send(one)

    mine = pl.ds(pl.multiple_of(c * COLS, COLS), COLS)
    missing = pl.ds(pl.multiple_of((1 - c) * COLS, COLS), COLS)

    def features(at):
        return pl.ds(pl.multiple_of(at * 512, 512), 512)

    def fetch(k):
        to = g_behind[k]
        push(w.at[mine, features(to)], wx.at[g, mine], hs, hr.at[k], at_g(to)).start()

    def hand_over(k):
        block = wx.at[g_ahead[k], mine]
        push(block, block, hs, hr.at[k], at_g(g_ahead[k])).wait_recv()
        push(block, block, ks, kr.at[k], {"dp_1": 1 - c}).start()

    for k in EARLY:
        fetch(k)

    own_rows = rows(d)
    pieces = [along(hop, 4, pair) for hop in HOPS]
    for j, i in enumerate(pieces):
        if j == 0:
            pre(6, 12)
        for one in (mate,) if HOPS[j] == 0 else (2 * i, 2 * i + 1):
            u_wait(one)
        for which in range(2):
            part = slice(which * COLS, (which + 1) * COLS)
            table = jnp.concatenate([tb[2 * i, part, :], tb[2 * i + 1, part, :]], axis=0)
            out[i, :, which] = dot(sel[...], table, NT).astype(BF16).reshape(PLANE, ROWS, DH)
        for k, dd in partners:
            d_to, g_to = d_ahead[dd], g_behind[k]
            push(
                out.at[i, d_to * 8 + g_to], pp.at[i, g, :, own_rows, :], ps, pr.at[j, k], device(d_to, g_to)
            ).start()
        for which in range(2):
            pp[i, g, which, own_rows, :] = out[i, me, which]
    pre(18, 14)
    for k in EARLY:
        hand_over(k)

    def head(i, g_here):
        h = g_here * 4 + i
        lanes = pl.ds(pl.multiple_of(h * DH, DH), DH)
        q, cot = qv[:, lanes], cv[:, lanes]
        scores = dot(pp[i, g_here, 0], q, NT) * SCALE
        grad = dot(pp[i, g_here, 1], cot, NT)
        self_top = stat[h, 0:1]
        top = jnp.maximum(jnp.max(scores, axis=0, keepdims=True), self_top)
        exponent = jnp.exp(scores - top)
        shrink = jnp.exp(self_top - top)
        inverse = 1.0 / (shrink * stat[h, 1:2] + jnp.sum(exponent, axis=0, keepdims=True))
        attention = exponent * inverse
        self_scale = shrink * inverse
        stat[h, 3:4] = self_scale
        rounded = attention.astype(BF16)
        pat[h] = rounded
        inner = self_scale * stat[h, 2:3] + jnp.sum(attention * grad, axis=0, keepdims=True)
        grad_scores = (attention * (grad - inner)).astype(BF16)
        gg[i, g_here, 0] = (dot(grad_scores, q) * SCALE).astype(BF16)
        gg[i, g_here, 1] = dot(rounded, cot).astype(BF16)

    def mid_step(j, i, ks, own_first):
        groups = [along(k, 8, g) for k in ks]
        for n, (k, g_here) in enumerate(zip(ks, groups)):
            if own_first and n == 0:
                drain(pp.at[i, g_here, :, pl.ds(0, PTOK - ROWS), :], pr.at[j, k])
            else:
                drain(pp.at[i, g_here], pr.at[j, k])
        for g_here in groups:
            head(i, g_here)
        for n, g_here in enumerate(groups):
            for dd in range(1 if own_first and n == 0 else 0, 4):
                d_to = d_ahead[dd]
                push(
                    gg.at[i, g_here, :, rows(d_to), :], rg.at[i, me], gs, gr.at[j], device(d_to, g_here)
                ).start()

    for j in MID:
        i = pieces[j]
        mid_step(j, i, list(range(MID_HEADS)), True)
        rg[i, me] = gg[i, g, :, own_rows, :]

        def later(n, carry, j=j, i=i):
            mid_step(j, i, [n * MID_HEADS + e for e in range(MID_HEADS)], False)
            return carry

        lax.fori_loop(1, 8 // MID_HEADS, later, 0)

    def post(first, count):
        def step(n, carry):
            for e in range(POST_HEADS):
                h = first + n * POST_HEADS + e
                lanes = pl.ds(pl.multiple_of(h * DH, DH), DH)
                self_part = (self_e[h] * stat[h, 3:4]).astype(BF16)
                prompt_values = pp[lax.rem(h, 4), lax.div(h, 4), 1]
                summed = dot(self_part, vv[:, lanes], TN) + dot(pat[h], prompt_values, TN)
                attended[:, lanes] = summed.astype(BF16)
            return carry

        lax.fori_loop(0, count // POST_HEADS, step, 0)

    for k in LATE:
        fetch(k)
    post(0, 8)

    for j in MID:
        i = pieces[j]
        drain(rg.at[i, pl.ds(0, PLANE - 1)], gr.at[j])
        for which in range(2):
            summed = dot(rg[i, :, which].reshape(PLANE * ROWS, DH), sel[...], TN).astype(BF16)
            part = slice(which * COLS, (which + 1) * COLS)
            gz[2 * i, part, :] = summed[:COLS]
            gz[2 * i + 1, part, :] = summed[COLS:]
        for to in (mate,) if HOPS[j] == 0 else (2 * i, 2 * i + 1):
            push(gz.at[to], rz.at[along(to - z, 8, 0)], bs, br, at_z(to)).start()
    for k in LATE:
        hand_over(k)
    post(8, 8)
    grad = gz[z].astype(F32)
    drain(rz.at[pl.ds(1, 7)], br)
    for o in range(1, 8):
        grad += rz[o].astype(F32)
    gt[g] = grad.astype(BF16)

    for k in reversed(NEAR):
        push(gt.at[g], gt.at[g], cs, cr.at[k], at_g(g_behind[k])).start()
    post(16, 10)
    terms = dot(w[:, features(g)], gt[g], TN)
    for k in NEAR:
        source = g_ahead[k]
        block = wx.at[source, missing]
        push(block, block, ks, kr.at[k], {"dp_1": 1 - c}).wait_recv()
        push(gt.at[source], gt.at[source], cs, cr.at[k], at_g(source)).wait_recv()
        terms += dot(wx[source], gt[source], TN)
    t2[...] = terms.astype(BF16).reshape(8, COLS, 128)
    for o in reversed(RING):
        to = along(o, 8, z)
        push(t2.at[to], rz2.at[o], es, er, at_z(to)).start()
    post(26, 6)
    mix = soft(logits[...])
    mixture_grad = t2[z].astype(F32)
    drain(rz2.at[pl.ds(1, 7)], er)
    for o in range(1, 8):
        mixture_grad += rz2[o].astype(F32)

    flipped = mixture_grad.T
    high = flipped.astype(BF16).astype(F32)
    middle = (flipped - high).astype(BF16).astype(F32)
    low = flipped - high - middle
    part = jnp.zeros((4 * NTASK, NSRC), F32)
    for r in range(ROWS):
        these = slice(r * NTASK, (r + 1) * NTASK)
        terms = jnp.concatenate([high[these], middle[these], low[these], jnp.zeros_like(low[these])], axis=0)
        part += dot(terms.astype(BF16), spv[r])
    part = part[:NTASK] + part[NTASK : 2 * NTASK] + part[2 * NTASK : 3 * NTASK]
    wslot[me] = part

    for k, dd in partners:
        push(wslot.at[me], wslot.at[me], ws, wr, device(d_ahead[dd], g_behind[k])).start()
    tile = jnp.concatenate([mix] * ROWS, axis=0)
    lane = lax.broadcasted_iota(jnp.int32, (COLS, 128), 1)
    for r in range(ROWS):
        chosen = jnp.where(lane // NTASK == r, mixture_grad, 0.0)
        source_grad[r] = jnp.dot(chosen, tile, precision=HIGH, preferred_element_type=F32)
    drain(wslot.at[pl.ds(0, PLANE - 1)], wr)
    wz[z] = jnp.sum(wslot[...], axis=0)
    for o in reversed(RING):
        push(wz.at[z], wz.at[z], vs, vr, at_z(along(o, 8, z))).start()
    drain(mix_t.at[0, y, z], xs)
    drain(mix_t.at[:, y, pl.ds(0, 7)], zs)
    drain(mix_t.at[:, pl.ds(0, 2)], ys)
    drain(mix_t.at[:, y], qs)
    drain(tt.at[pl.ds(0, PLANE - 1)], ts)
    drain(tb.at[pl.ds(0, 7)], us)
    drain(out.at[:, pl.ds(0, PLANE - 1)], ps)
    drain(rg.at[:, pl.ds(0, PLANE - 1)], gs)
    drain(gz.at[pl.ds(0, 7)], bs)
    drain(wx.at[pl.ds(0, 7), mine], hs)
    drain(wx.at[pl.ds(0, 7), mine], ks)
    drain(gt.at[pl.ds(0, 7)], cs)
    drain(t2.at[pl.ds(0, 7)], es)
    drain(wslot.at[pl.ds(0, PLANE - 1)], ws)
    drain(wz.at[pl.ds(0, 7)], vr)
    weight_grad = jnp.sum(wz[...], axis=0)
    logits_grad[...] = mix * (weight_grad - jnp.sum(mix * weight_grad, axis=1, keepdims=True))
    drain(wz.at[pl.ds(0, 7)], vs)


def on_device(source_prompts, task_logits, task_ids, key_weight, value_weight, queries, keys, values, cotangent):
    any_space = pl.BlockSpec(memory_space=pl.ANY)
    vmem = pl.BlockSpec(memory_space=pltpu.VMEM)
    dma = pltpu.SemaphoreType.DMA
    attended, source_grad, logits_grad = pl.pallas_call(
        kernel,
        out_shape=(
            pltpu.VMEM((SEQ, D), BF16),
            pltpu.VMEM((ROWS, COLS, NSRC), F32),
            pltpu.VMEM((NTASK, NSRC), F32),
        ),
        in_specs=[pl.BlockSpec(memory_space=pltpu.SMEM), vmem] + [any_space] * 7,
        out_specs=(vmem, vmem, vmem),
        scratch_shapes=[
            pltpu.VMEM((ROWS, COLS, NSRC), BF16),
            pltpu.VMEM((2 * COLS, D), BF16),
            pltpu.VMEM((8, 2 * COLS, 512), BF16),
            *[pltpu.VMEM((SEQ, D), BF16)] * 4,
            pltpu.VMEM((2, 4, 8, COLS, 128), BF16),
            pltpu.VMEM((8, 128, 128), BF16),
            pltpu.VMEM((PLANE, 8, 128), F32),
            pltpu.VMEM((PLANE * ROWS, 128), BF16),
            pltpu.VMEM((4, PLANE, 2, ROWS, DH), BF16),
            pltpu.VMEM((4, 8, 2, PTOK, DH), BF16),
            pltpu.VMEM((HEADS, 8, SEQ), F32),
            pltpu.VMEM((HEADS, SEQ, SEQ), F32),
            pltpu.VMEM((HEADS, PTOK, SEQ), BF16),
            pltpu.VMEM((4, 8, 2, PTOK, DH), BF16),
            pltpu.VMEM((4, PLANE, 2, ROWS, DH), BF16),
            pltpu.VMEM((8, 128, 128), BF16),
            pltpu.VMEM((8, 128, 128), BF16),
            pltpu.VMEM((8, 128, 128), BF16),
            pltpu.VMEM((8, COLS, 128), BF16),
            pltpu.VMEM((8, COLS, 128), BF16),
            pltpu.VMEM((PLANE, NTASK, NSRC), F32),
            pltpu.VMEM((8, NTASK, NSRC), F32),
            dma((7,)), dma, dma((2, 8)), dma, dma, dma, dma((2, 2, 8)), dma, dma((2,)), dma, dma((8,)),
            dma, dma, dma, dma((4, 8)), dma, dma((4,)), dma, dma((8,)), dma, dma((8,)),
            dma, dma, dma, dma((8,)), dma, dma,
            dma, dma, dma, dma,
        ],
        compiler_params=pltpu.CompilerParams(collective_id=0, has_side_effects=True),
        name="prompt_step",
    )(
        task_ids, task_logits, source_prompts.transpose(1, 2, 0), key_weight.T, value_weight.T,
        queries[0], keys[0], values[0], cotangent[0],
    )
    return attended[None], source_grad.transpose(2, 0, 1), logits_grad


def solution(mesh):
    torus = Mesh(mesh.devices.reshape(2, 2, 2, 4, 8), AXES)
    return jax.shard_map(
        on_device,
        mesh=torus,
        in_specs=(
            P(None, None, MP),
            P(),
            P(DP),
            P(None, MP),
            P(None, MP),
            P(AXES, None, None),
            P(AXES, None, None),
            P(AXES, None, None),
            P(AXES, None, None),
        ),
        out_specs=(P(AXES, None, None), P(None, DP, MP), P()),
        check_vma=False,
    )
```

```python
import jax
import jax.numpy as jnp
from jax import lax
from jax.experimental import pallas as pl
from jax.experimental.pallas import tpu as pltpu
from jax.sharding import Mesh
from jax.sharding import PartitionSpec as P

D = 4096
HEADS = 32
DH = 128
NSRC = 128
NTASK = 8
PTOK = 64
SEQ = 128
AXES = ("dp_0", "dp_1", "mp_0", "mp_1", "mp_2")
MP = ("mp_0", "mp_1", "mp_2")
DP = ("dp_0", "dp_1")
MESH = pl.DeviceIdType.MESH
ROWS = 16
COLS = 64
PLANE = 32
F32 = jnp.float32
BF16 = jnp.bfloat16
HIGH = lax.Precision.HIGHEST


def here():
    return tuple(lax.axis_index(name) for name in AXES)


def push(src, dst, sent, landed, device):
    return pltpu.make_async_remote_copy(
        src_ref=src, dst_ref=dst, send_sem=sent, recv_sem=landed, device_id=device, device_id_type=MESH
    )


def drain(ref, sem):
    pltpu.make_async_copy(ref, ref, sem).wait()


def far(partner):
    k, dd = partner
    return min(k % 4, 4 - k % 4) + (dd // 2) * 2 + k // 4


def soft(logits):
    exponent = jnp.exp(logits - jnp.max(logits, axis=1, keepdims=True))
    return exponent / jnp.sum(exponent, axis=1, keepdims=True)


NN = (((1,), (0,)), ((), ()))
NT = (((1,), (1,)), ((), ()))
TN = (((0,), (0,)), ((), ()))
SCALE = DH ** (-0.5)
HOPS = (0, 1, 3, 2)
MID = (1, 2, 3, 0)
RING = (1, 7, 2, 6, 3, 5, 4)
NEAR = (4, 1, 7, 3, 5, 2, 6)
EARLY, LATE = (1, 7, 4, 3), (2, 6, 5)
PRE_HEADS = 2
MID_HEADS = 2
POST_HEADS = 2


def dot(a, b, dims=NN):
    return lax.dot_general(a, b, dims, preferred_element_type=F32)


def kernel(
    tids, logits, sp, kw, vw, queries, keys, values, cotangent,
    attended, source_grad, logits_grad,
    spv, w, wx, qv, kv, vv, cv, mix_t, tb, tt, sel, out, pp, stat, self_e, pat, gg, rg, gz, rz, gt, t2, rz2,
    wslot, wz,
    load_sem, zs, zr, xs, xr, ys, yr, qs, qr, us, ur, ts, tr, ps, pr, gs, gr, hs, hr, ks, kr, bs, br, cs, cr, es, er,
    ws, wr, vs, vr,
):
    a, c, x, y, z = here()
    d, g = a * 2 + c, x * 4 + y
    me = d * 8 + g
    pair = lax.div(z, 2)
    barrier = pltpu.get_barrier_semaphore()

    def along(o, n, at):
        return lax.rem(at + o + n, n)

    d_ahead = [along(k, 4, d) for k in range(4)]
    d_behind = [along(-k, 4, d) for k in range(4)]
    g_behind = [along(-k, 8, g) for k in range(8)]
    g_ahead = [along(k, 8, g) for k in range(8)]
    partners = [(k, dd) for k in range(8) for dd in range(4)][1:]

    def device(d_to, g_to):
        return {
            "dp_0": lax.div(d_to, 2), "dp_1": lax.rem(d_to, 2), "mp_0": lax.div(g_to, 4), "mp_1": lax.rem(g_to, 4),
        }

    def at_z(to):
        return {"mp_2": to}

    def at_g(to):
        return {"mp_0": lax.div(to, 4), "mp_1": lax.rem(to, 4)}

    def at_y(to):
        return {"mp_1": to}

    other = 1 - x
    x_peer = {"mp_0": other}

    def rows(quarter):
        return pl.ds(pl.multiple_of(quarter * ROWS, ROWS), ROWS)

    loads = [
        pltpu.make_async_copy(sp.at[pl.ds(d * ROWS, ROWS)], spv, load_sem.at[0]),
        pltpu.make_async_copy(queries, qv, load_sem.at[1]),
        pltpu.make_async_copy(keys, kv, load_sem.at[2]),
        pltpu.make_async_copy(cotangent, cv, load_sem.at[3]),
        pltpu.make_async_copy(values, vv, load_sem.at[4]),
        pltpu.make_async_copy(kw, w.at[pl.ds(0, COLS)], load_sem.at[5]),
        pltpu.make_async_copy(vw, w.at[pl.ds(COLS, COLS)], load_sem.at[6]),
    ]
    loads[0].start()
    for o in reversed(RING):
        pl.semaphore_signal(barrier, inc=1, device_id=at_z(along(o, 8, z)), device_id_type=MESH)
    for k, dd in sorted(partners, key=far, reverse=True):
        pl.semaphore_signal(barrier, inc=1, device_id=device(d_ahead[dd], g_behind[k]), device_id_type=MESH)
    for load in loads[1:]:
        load.start()
    tt[me] = jnp.full((8, 128), tids[x * 32 + y * 8 + z], jnp.int32).astype(F32)
    tile = jnp.concatenate([soft(logits[...]).astype(BF16).astype(F32)] * ROWS, axis=0)
    row = lax.broadcasted_iota(jnp.int32, (128, 128), 0)
    loads[0].wait()
    total = jnp.zeros((COLS, 128), F32)
    for r in range(ROWS):
        weights = jnp.where(row // NTASK == r, tile, 0.0).astype(BF16)
        total += dot(spv[r], weights, NT)
    mix_t[x, y, z] = total.astype(BF16)
    pl.semaphore_wait(barrier, PLANE - 1 + 7)

    own = mix_t.at[x, y, z]
    push(own, own, xs, xr, x_peer).start()
    for o in RING:
        push(own, own, zs, zr.at[0, o], at_z(along(o, 8, z))).start()
    for k, dd in partners:
        push(tt.at[me], tt.at[me], ts, tr, device(d_ahead[dd], g_behind[k])).start()
    own = mix_t.at[other, y, z]
    push(own, own, xs, xr, x_peer).wait_recv()
    for o in RING:
        push(own, own, zs, zr.at[1, o], at_z(along(o, 8, z))).start()

    def pre(first, count):
        masked = lax.broadcasted_iota(jnp.int32, (SEQ, SEQ), 0) > lax.broadcasted_iota(jnp.int32, (SEQ, SEQ), 1)

        def step(n, carry):
            for e in range(PRE_HEADS):
                h = first + n * PRE_HEADS + e
                lanes = pl.ds(pl.multiple_of(h * DH, DH), DH)
                scores = dot(kv[:, lanes], qv[:, lanes], NT) * SCALE
                scores = jnp.where(masked, -1e30, scores)
                top = jnp.max(scores, axis=0, keepdims=True)
                exponent = jnp.exp(scores - top)
                grad = dot(vv[:, lanes], cv[:, lanes], NT)
                self_e[h] = exponent
                stat[h, 0:1] = top
                stat[h, 1:2] = jnp.sum(exponent, axis=0, keepdims=True)
                stat[h, 2:3] = jnp.sum(exponent * grad, axis=0, keepdims=True)
            return carry

        lax.fori_loop(0, count // PRE_HEADS, step, 0)

    for load in loads[1:5]:
        load.wait()
    up, down, across = along(1, 4, y), along(-1, 4, y), along(2, 4, y)
    halves = (x, other)

    def project(half, at):
        columns = pl.ds(pl.multiple_of(half * 2048 + at * 512, 512), 512)
        return dot(w[:, columns], mix_t[half, at].reshape(512, 128))

    def y_push(n, half, o):
        block = mix_t.at[half, y, along(-o, 8, z)]
        push(block, block, ys, yr.at[n, 0, o], at_y(up)).start()
        push(block, block, ys, yr.at[n, 1, o], at_y(down)).start()

    def y_relay(n, half, o, upward):
        source = along(-o, 8, z)
        from_down, from_up = mix_t.at[half, down, source], mix_t.at[half, up, source]
        push(from_down, from_down, ys, yr.at[n, 0, o], at_y(down)).wait_recv()
        if upward:
            push(from_down, from_down, qs, qr.at[n], at_y(up)).start()
        push(from_up, from_up, ys, yr.at[n, 1, o], at_y(up)).wait_recv()
        if not upward:
            push(from_up, from_up, qs, qr.at[n], at_y(down)).start()

    y_push(0, x, 0)
    y_push(1, other, 0)
    pre(0, 6)
    for o in RING:
        for n, half in enumerate(halves):
            block = mix_t.at[half, y, along(-o, 8, z)]
            push(block, block, zs, zr.at[n, o], at_z(along(-o, 8, z))).wait_recv()
            y_push(n, half, o)
    places = tuple(enumerate((0, *RING)))
    for place, o in places[:6]:
        for n, half in enumerate(halves):
            y_relay(n, half, o, place % 2 == 0)
    for load in loads[5:]:
        load.wait()
    total = project(x, y) + project(other, y)
    for place, o in places[6:]:
        for n, half in enumerate(halves):
            y_relay(n, half, o, place % 2 == 0)
    total += project(x, down) + project(x, up) + project(other, down) + project(other, up)

    drain(tt.at[pl.ds(0, PLANE - 1)], tr)
    lane = lax.broadcasted_iota(jnp.int32, (ROWS, 128), 1)
    prompt_row = lax.broadcasted_iota(jnp.int32, (ROWS, 128), 0)
    lane_task = (lane % NTASK).astype(F32)
    lane_row = lane // NTASK == prompt_row

    def select(p, carry):
        task = jnp.concatenate([tt[p], tt[p]], axis=0)
        hit = jnp.where(lane_row & (task == lane_task), 1.0, 0.0)
        sel[rows(p), :] = hit.astype(BF16)
        return carry

    lax.fori_loop(0, PLANE, select, 0)
    for n, half in enumerate(halves):
        drain(mix_t.at[half, across], qr.at[n])
        total += project(half, across)

    tb[z] = total.astype(BF16)
    mate = pair * 2 + 1 - lax.rem(z, 2)

    def u_send(to):
        push(tb.at[z], tb.at[z], us, ur.at[along(to - z, 8, 0)], at_z(to)).start()

    def u_wait(source):
        push(tb.at[source], tb.at[source], us, ur.at[along(z - source, 8, 0)], at_z(source)).wait_recv()

    for hop in HOPS:
        to = along(-hop, 4, pair)
        for one in (mate,) if hop == 0 else (2 * to, 2 * to + 1):
            u_send(one)

    mine = pl.ds(pl.multiple_of(c * COLS, COLS), COLS)
    missing = pl.ds(pl.multiple_of((1 - c) * COLS, COLS), COLS)

    def features(at):
        return pl.ds(pl.multiple_of(at * 512, 512), 512)

    def fetch(k):
        to = g_behind[k]
        push(w.at[mine, features(to)], wx.at[g, mine], hs, hr.at[k], at_g(to)).start()

    def hand_over(k):
        block = wx.at[g_ahead[k], mine]
        push(block, block, hs, hr.at[k], at_g(g_ahead[k])).wait_recv()
        push(block, block, ks, kr.at[k], {"dp_1": 1 - c}).start()

    for k in EARLY:
        fetch(k)

    own_rows = rows(d)
    pieces = [along(hop, 4, pair) for hop in HOPS]
    for j, i in enumerate(pieces):
        if j == 0:
            pre(6, 12)
        for one in (mate,) if HOPS[j] == 0 else (2 * i, 2 * i + 1):
            u_wait(one)
        for which in range(2):
            part = slice(which * COLS, (which + 1) * COLS)
            table = jnp.concatenate([tb[2 * i, part, :], tb[2 * i + 1, part, :]], axis=0)
            out[i, :, which] = dot(sel[...], table, NT).astype(BF16).reshape(PLANE, ROWS, DH)
        for k, dd in partners:
            d_to, g_to = d_ahead[dd], g_behind[k]
            push(
                out.at[i, d_to * 8 + g_to], pp.at[i, g, :, own_rows, :], ps, pr.at[j, k], device(d_to, g_to)
            ).start()
        for which in range(2):
            pp[i, g, which, own_rows, :] = out[i, me, which]
    pre(18, 14)
    for k in EARLY:
        hand_over(k)

    def head(i, g_here):
        h = g_here * 4 + i
        lanes = pl.ds(pl.multiple_of(h * DH, DH), DH)
        q, cot = qv[:, lanes], cv[:, lanes]
        scores = dot(pp[i, g_here, 0], q, NT) * SCALE
        grad = dot(pp[i, g_here, 1], cot, NT)
        self_top = stat[h, 0:1]
        top = jnp.maximum(jnp.max(scores, axis=0, keepdims=True), self_top)
        exponent = jnp.exp(scores - top)
        shrink = jnp.exp(self_top - top)
        inverse = 1.0 / (shrink * stat[h, 1:2] + jnp.sum(exponent, axis=0, keepdims=True))
        attention = exponent * inverse
        self_scale = shrink * inverse
        stat[h, 3:4] = self_scale
        rounded = attention.astype(BF16)
        pat[h] = rounded
        inner = self_scale * stat[h, 2:3] + jnp.sum(attention * grad, axis=0, keepdims=True)
        grad_scores = (attention * (grad - inner)).astype(BF16)
        gg[i, g_here, 0] = (dot(grad_scores, q) * SCALE).astype(BF16)
        gg[i, g_here, 1] = dot(rounded, cot).astype(BF16)

    def mid_step(j, i, ks, own_first):
        groups = [along(k, 8, g) for k in ks]
        for n, (k, g_here) in enumerate(zip(ks, groups)):
            if own_first and n == 0:
                drain(pp.at[i, g_here, :, pl.ds(0, PTOK - ROWS), :], pr.at[j, k])
            else:
                drain(pp.at[i, g_here], pr.at[j, k])
        for g_here in groups:
            head(i, g_here)
        for n, g_here in enumerate(groups):
            for dd in range(1 if own_first and n == 0 else 0, 4):
                d_to = d_ahead[dd]
                push(
                    gg.at[i, g_here, :, rows(d_to), :], rg.at[i, me], gs, gr.at[j], device(d_to, g_here)
                ).start()

    for j in MID:
        i = pieces[j]
        mid_step(j, i, list(range(MID_HEADS)), True)
        rg[i, me] = gg[i, g, :, own_rows, :]

        def later(n, carry, j=j, i=i):
            mid_step(j, i, [n * MID_HEADS + e for e in range(MID_HEADS)], False)
            return carry

        lax.fori_loop(1, 8 // MID_HEADS, later, 0)

    def post(first, count):
        def step(n, carry):
            for e in range(POST_HEADS):
                h = first + n * POST_HEADS + e
                lanes = pl.ds(pl.multiple_of(h * DH, DH), DH)
                self_part = (self_e[h] * stat[h, 3:4]).astype(BF16)
                prompt_values = pp[lax.rem(h, 4), lax.div(h, 4), 1]
                summed = dot(self_part, vv[:, lanes], TN) + dot(pat[h], prompt_values, TN)
                attended[:, lanes] = summed.astype(BF16)
            return carry

        lax.fori_loop(0, count // POST_HEADS, step, 0)

    for k in LATE:
        fetch(k)
    post(0, 8)

    for j in MID:
        i = pieces[j]
        drain(rg.at[i, pl.ds(0, PLANE - 1)], gr.at[j])
        for which in range(2):
            summed = dot(rg[i, :, which].reshape(PLANE * ROWS, DH), sel[...], TN).astype(BF16)
            part = slice(which * COLS, (which + 1) * COLS)
            gz[2 * i, part, :] = summed[:COLS]
            gz[2 * i + 1, part, :] = summed[COLS:]
        for to in (mate,) if HOPS[j] == 0 else (2 * i, 2 * i + 1):
            push(gz.at[to], rz.at[along(to - z, 8, 0)], bs, br, at_z(to)).start()
    for k in LATE:
        hand_over(k)
    post(8, 8)
    grad = gz[z].astype(F32)
    drain(rz.at[pl.ds(1, 7)], br)
    for o in range(1, 8):
        grad += rz[o].astype(F32)
    gt[g] = grad.astype(BF16)

    for k in reversed(NEAR):
        push(gt.at[g], gt.at[g], cs, cr.at[k], at_g(g_behind[k])).start()
    post(16, 10)
    terms = dot(w[:, features(g)], gt[g], TN)
    for k in NEAR:
        source = g_ahead[k]
        block = wx.at[source, missing]
        push(block, block, ks, kr.at[k], {"dp_1": 1 - c}).wait_recv()
        push(gt.at[source], gt.at[source], cs, cr.at[k], at_g(source)).wait_recv()
        terms += dot(wx[source], gt[source], TN)
    t2[...] = terms.astype(BF16).reshape(8, COLS, 128)
    for o in reversed(RING):
        to = along(o, 8, z)
        push(t2.at[to], rz2.at[o], es, er, at_z(to)).start()
    post(26, 6)
    mix = soft(logits[...])
    mixture_grad = t2[z].astype(F32)
    drain(rz2.at[pl.ds(1, 7)], er)
    for o in range(1, 8):
        mixture_grad += rz2[o].astype(F32)

    flipped = mixture_grad.T
    high = flipped.astype(BF16).astype(F32)
    middle = (flipped - high).astype(BF16).astype(F32)
    low = flipped - high - middle
    part = jnp.zeros((4 * NTASK, NSRC), F32)
    for r in range(ROWS):
        these = slice(r * NTASK, (r + 1) * NTASK)
        terms = jnp.concatenate([high[these], middle[these], low[these], jnp.zeros_like(low[these])], axis=0)
        part += dot(terms.astype(BF16), spv[r])
    part = part[:NTASK] + part[NTASK : 2 * NTASK] + part[2 * NTASK : 3 * NTASK]
    wslot[me] = part

    for k, dd in partners:
        push(wslot.at[me], wslot.at[me], ws, wr, device(d_ahead[dd], g_behind[k])).start()
    tile = jnp.concatenate([mix] * ROWS, axis=0)
    lane = lax.broadcasted_iota(jnp.int32, (COLS, 128), 1)
    for r in range(ROWS):
        chosen = jnp.where(lane // NTASK == r, mixture_grad, 0.0)
        source_grad[r] = jnp.dot(chosen, tile, precision=HIGH, preferred_element_type=F32)
    drain(wslot.at[pl.ds(0, PLANE - 1)], wr)
    wz[z] = jnp.sum(wslot[...], axis=0)
    for o in reversed(RING):
        push(wz.at[z], wz.at[z], vs, vr, at_z(along(o, 8, z))).start()
    drain(mix_t.at[0, y, z], xs)
    drain(mix_t.at[:, y, pl.ds(0, 7)], zs)
    drain(mix_t.at[:, pl.ds(0, 2)], ys)
    drain(mix_t.at[:, y], qs)
    drain(tt.at[pl.ds(0, PLANE - 1)], ts)
    drain(tb.at[pl.ds(0, 7)], us)
    drain(out.at[:, pl.ds(0, PLANE - 1)], ps)
    drain(rg.at[:, pl.ds(0, PLANE - 1)], gs)
    drain(gz.at[pl.ds(0, 7)], bs)
    drain(wx.at[pl.ds(0, 7), mine], hs)
    drain(wx.at[pl.ds(0, 7), mine], ks)
    drain(gt.at[pl.ds(0, 7)], cs)
    drain(t2.at[pl.ds(0, 7)], es)
    drain(wslot.at[pl.ds(0, PLANE - 1)], ws)
    drain(wz.at[pl.ds(0, 7)], vr)
    weight_grad = jnp.sum(wz[...], axis=0)
    logits_grad[...] = mix * (weight_grad - jnp.sum(mix * weight_grad, axis=1, keepdims=True))
    drain(wz.at[pl.ds(0, 7)], vs)


def finish_kernel(attended, source_grad, logits_grad, attended_out, source_out, logits_out, sems):
    given = ((attended, attended_out), (source_grad, source_out), (logits_grad, logits_out))
    copies = [pltpu.make_async_copy(one, to, sems.at[n]) for n, (one, to) in enumerate(given)]
    for one in copies:
        one.start()
    for one in copies:
        one.wait()


def finish(*given):
    vmem = pl.BlockSpec(memory_space=pltpu.VMEM)
    any_space = pl.BlockSpec(memory_space=pl.ANY)
    return pl.pallas_call(
        finish_kernel,
        out_shape=tuple(jax.ShapeDtypeStruct(one.shape, one.dtype) for one in given),
        in_specs=[vmem] * 3,
        out_specs=(any_space,) * 3,
        scratch_shapes=[pltpu.SemaphoreType.DMA((3,))],
        name="prompt_finish",
    )(*(pltpu.with_memory_space_constraint(one, pltpu.VMEM) for one in given))


def on_device(source_prompts, task_logits, task_ids, key_weight, value_weight, queries, keys, values, cotangent):
    any_space = pl.BlockSpec(memory_space=pl.ANY)
    vmem = pl.BlockSpec(memory_space=pltpu.VMEM)
    dma = pltpu.SemaphoreType.DMA
    attended, source_grad, logits_grad = pl.pallas_call(
        kernel,
        out_shape=(
            pltpu.VMEM((SEQ, D), BF16),
            pltpu.VMEM((ROWS, COLS, NSRC), F32),
            pltpu.VMEM((NTASK, NSRC), F32),
        ),
        in_specs=[pl.BlockSpec(memory_space=pltpu.SMEM), vmem] + [any_space] * 7,
        out_specs=(vmem, vmem, vmem),
        scratch_shapes=[
            pltpu.VMEM((ROWS, COLS, NSRC), BF16),
            pltpu.VMEM((2 * COLS, D), BF16),
            pltpu.VMEM((8, 2 * COLS, 512), BF16),
            *[pltpu.VMEM((SEQ, D), BF16)] * 4,
            pltpu.VMEM((2, 4, 8, COLS, 128), BF16),
            pltpu.VMEM((8, 128, 128), BF16),
            pltpu.VMEM((PLANE, 8, 128), F32),
            pltpu.VMEM((PLANE * ROWS, 128), BF16),
            pltpu.VMEM((4, PLANE, 2, ROWS, DH), BF16),
            pltpu.VMEM((4, 8, 2, PTOK, DH), BF16),
            pltpu.VMEM((HEADS, 8, SEQ), F32),
            pltpu.VMEM((HEADS, SEQ, SEQ), F32),
            pltpu.VMEM((HEADS, PTOK, SEQ), BF16),
            pltpu.VMEM((4, 8, 2, PTOK, DH), BF16),
            pltpu.VMEM((4, PLANE, 2, ROWS, DH), BF16),
            pltpu.VMEM((8, 128, 128), BF16),
            pltpu.VMEM((8, 128, 128), BF16),
            pltpu.VMEM((8, 128, 128), BF16),
            pltpu.VMEM((8, COLS, 128), BF16),
            pltpu.VMEM((8, COLS, 128), BF16),
            pltpu.VMEM((PLANE, NTASK, NSRC), F32),
            pltpu.VMEM((8, NTASK, NSRC), F32),
            dma((7,)), dma, dma((2, 8)), dma, dma, dma, dma((2, 2, 8)), dma, dma((2,)), dma, dma((8,)),
            dma, dma, dma, dma((4, 8)), dma, dma((4,)), dma, dma((8,)), dma, dma((8,)),
            dma, dma, dma, dma((8,)), dma, dma,
            dma, dma, dma, dma,
        ],
        compiler_params=pltpu.CompilerParams(collective_id=0, has_side_effects=True),
        name="prompt_step",
    )(
        task_ids, task_logits, source_prompts.transpose(1, 2, 0), key_weight.T, value_weight.T,
        queries[0], keys[0], values[0], cotangent[0],
    )
    attended, source_grad, logits_grad = finish(attended, source_grad, logits_grad)
    return attended[None], source_grad.transpose(2, 0, 1), logits_grad


def solution(mesh):
    torus = Mesh(mesh.devices.reshape(2, 2, 2, 4, 8), AXES)
    return jax.shard_map(
        on_device,
        mesh=torus,
        in_specs=(
            P(None, None, MP),
            P(),
            P(DP),
            P(None, MP),
            P(None, MP),
            P(AXES, None, None),
            P(AXES, None, None),
            P(AXES, None, None),
            P(AXES, None, None),
        ),
        out_specs=(P(AXES, None, None), P(None, DP, MP), P()),
        check_vma=False,
    )
```

```python
import jax
import jax.numpy as jnp
from jax import lax
from jax.experimental import pallas as pl
from jax.experimental.pallas import tpu as pltpu
from jax.sharding import Mesh
from jax.sharding import PartitionSpec as P

D = 4096
HEADS = 32
DH = 128
NSRC = 128
NTASK = 8
PTOK = 64
SEQ = 128
AXES = ("dp_0", "dp_1", "mp_0", "mp_1", "mp_2")
MP = ("mp_0", "mp_1", "mp_2")
DP = ("dp_0", "dp_1")
MESH = pl.DeviceIdType.MESH
ROWS = 16
COLS = 64
PLANE = 32
F32 = jnp.float32
BF16 = jnp.bfloat16
HIGH = lax.Precision.HIGHEST


def here():
    return tuple(lax.axis_index(name) for name in AXES)


def push(src, dst, sent, landed, device):
    return pltpu.make_async_remote_copy(
        src_ref=src, dst_ref=dst, send_sem=sent, recv_sem=landed, device_id=device, device_id_type=MESH
    )


def drain(ref, sem):
    pltpu.make_async_copy(ref, ref, sem).wait()


def far(partner):
    k, dd = partner
    return min(k % 4, 4 - k % 4) + (dd // 2) * 2 + k // 4


def soft(logits):
    exponent = jnp.exp(logits - jnp.max(logits, axis=1, keepdims=True))
    return exponent / jnp.sum(exponent, axis=1, keepdims=True)


NN = (((1,), (0,)), ((), ()))
NT = (((1,), (1,)), ((), ()))
TN = (((0,), (0,)), ((), ()))
SCALE = DH ** (-0.5)
HOPS = (0, 1, 3, 2)
MID = (1, 2, 3, 0)
RING = (1, 7, 2, 6, 3, 5, 4)
NEAR = (4, 1, 7, 3, 5, 2, 6)
EARLY, LATE = (1, 7, 4, 3), (2, 6, 5)
PRE_HEADS = 2
MID_HEADS = 4
POST_HEADS = 2


def dot(a, b, dims=NN):
    return lax.dot_general(a, b, dims, preferred_element_type=F32)


def kernel(
    tids, logits, sp, kw, vw, queries, keys, values, cotangent,
    attended, source_grad, logits_grad,
    spv, w, wx, qv, kv, vv, cv, mix_t, tb, tt, sel, out, pp, stat, self_e, pat, gg, rg, gz, rz, gt, t2, rz2,
    wslot, wz,
    load_sem, zs, zr, xs, xr, ys, yr, qs, qr, us, ur, ts, tr, ps, pr, gs, gr, hs, hr, ks, kr, bs, br, cs, cr, es, er,
    ws, wr, vs, vr,
):
    a, c, x, y, z = here()
    d, g = a * 2 + c, x * 4 + y
    me = d * 8 + g
    pair = lax.div(z, 2)
    barrier = pltpu.get_barrier_semaphore()

    def along(o, n, at):
        return lax.rem(at + o + n, n)

    d_ahead = [along(k, 4, d) for k in range(4)]
    d_behind = [along(-k, 4, d) for k in range(4)]
    g_behind = [along(-k, 8, g) for k in range(8)]
    g_ahead = [along(k, 8, g) for k in range(8)]
    partners = [(k, dd) for k in range(8) for dd in range(4)][1:]

    def device(d_to, g_to):
        return {
            "dp_0": lax.div(d_to, 2), "dp_1": lax.rem(d_to, 2), "mp_0": lax.div(g_to, 4), "mp_1": lax.rem(g_to, 4),
        }

    def at_z(to):
        return {"mp_2": to}

    def at_g(to):
        return {"mp_0": lax.div(to, 4), "mp_1": lax.rem(to, 4)}

    def at_y(to):
        return {"mp_1": to}

    other = 1 - x
    x_peer = {"mp_0": other}

    def rows(quarter):
        return pl.ds(pl.multiple_of(quarter * ROWS, ROWS), ROWS)

    loads = [
        pltpu.make_async_copy(sp.at[pl.ds(d * ROWS, ROWS)], spv, load_sem.at[0]),
        pltpu.make_async_copy(queries, qv, load_sem.at[1]),
        pltpu.make_async_copy(keys, kv, load_sem.at[2]),
        pltpu.make_async_copy(cotangent, cv, load_sem.at[3]),
        pltpu.make_async_copy(values, vv, load_sem.at[4]),
        pltpu.make_async_copy(kw, w.at[pl.ds(0, COLS)], load_sem.at[5]),
        pltpu.make_async_copy(vw, w.at[pl.ds(COLS, COLS)], load_sem.at[6]),
    ]
    loads[0].start()
    for o in reversed(RING):
        pl.semaphore_signal(barrier, inc=1, device_id=at_z(along(o, 8, z)), device_id_type=MESH)
    for k, dd in sorted(partners, key=far, reverse=True):
        pl.semaphore_signal(barrier, inc=1, device_id=device(d_ahead[dd], g_behind[k]), device_id_type=MESH)
    for load in loads[1:]:
        load.start()
    tt[me] = jnp.full((8, 128), tids[x * 32 + y * 8 + z], jnp.int32).astype(F32)
    tile = jnp.concatenate([soft(logits[...]).astype(BF16).astype(F32)] * ROWS, axis=0)
    row = lax.broadcasted_iota(jnp.int32, (128, 128), 0)
    loads[0].wait()
    total = jnp.zeros((COLS, 128), F32)
    for r in range(ROWS):
        weights = jnp.where(row // NTASK == r, tile, 0.0).astype(BF16)
        total += dot(spv[r], weights, NT)
    mix_t[x, y, z] = total.astype(BF16)
    pl.semaphore_wait(barrier, PLANE - 1 + 7)

    own = mix_t.at[x, y, z]
    push(own, own, xs, xr, x_peer).start()
    for o in RING:
        push(own, own, zs, zr.at[0, o], at_z(along(o, 8, z))).start()
    for k, dd in partners:
        push(tt.at[me], tt.at[me], ts, tr, device(d_ahead[dd], g_behind[k])).start()
    own = mix_t.at[other, y, z]
    push(own, own, xs, xr, x_peer).wait_recv()
    for o in RING:
        push(own, own, zs, zr.at[1, o], at_z(along(o, 8, z))).start()

    def pre(first, count):
        masked = lax.broadcasted_iota(jnp.int32, (SEQ, SEQ), 0) > lax.broadcasted_iota(jnp.int32, (SEQ, SEQ), 1)

        def step(n, carry):
            for e in range(PRE_HEADS):
                h = first + n * PRE_HEADS + e
                lanes = pl.ds(pl.multiple_of(h * DH, DH), DH)
                scores = dot(kv[:, lanes], qv[:, lanes], NT) * SCALE
                scores = jnp.where(masked, -1e30, scores)
                top = jnp.max(scores, axis=0, keepdims=True)
                exponent = jnp.exp(scores - top)
                grad = dot(vv[:, lanes], cv[:, lanes], NT)
                self_e[h] = exponent
                stat[h, 0:1] = top
                stat[h, 1:2] = jnp.sum(exponent, axis=0, keepdims=True)
                stat[h, 2:3] = jnp.sum(exponent * grad, axis=0, keepdims=True)
            return carry

        lax.fori_loop(0, count // PRE_HEADS, step, 0)

    for load in loads[1:5]:
        load.wait()
    up, down, across = along(1, 4, y), along(-1, 4, y), along(2, 4, y)
    halves = (x, other)

    def project(half, at):
        columns = pl.ds(pl.multiple_of(half * 2048 + at * 512, 512), 512)
        return dot(w[:, columns], mix_t[half, at].reshape(512, 128))

    def y_push(n, half, o):
        block = mix_t.at[half, y, along(-o, 8, z)]
        push(block, block, ys, yr.at[n, 0, o], at_y(up)).start()
        push(block, block, ys, yr.at[n, 1, o], at_y(down)).start()

    def y_relay(n, half, o, upward):
        source = along(-o, 8, z)
        from_down, from_up = mix_t.at[half, down, source], mix_t.at[half, up, source]
        push(from_down, from_down, ys, yr.at[n, 0, o], at_y(down)).wait_recv()
        if upward:
            push(from_down, from_down, qs, qr.at[n], at_y(up)).start()
        push(from_up, from_up, ys, yr.at[n, 1, o], at_y(up)).wait_recv()
        if not upward:
            push(from_up, from_up, qs, qr.at[n], at_y(down)).start()

    y_push(0, x, 0)
    y_push(1, other, 0)
    pre(0, 6)
    for o in RING:
        for n, half in enumerate(halves):
            block = mix_t.at[half, y, along(-o, 8, z)]
            push(block, block, zs, zr.at[n, o], at_z(along(-o, 8, z))).wait_recv()
            y_push(n, half, o)
    places = tuple(enumerate((0, *RING)))
    for place, o in places[:6]:
        for n, half in enumerate(halves):
            y_relay(n, half, o, place % 2 == 0)
    for load in loads[5:]:
        load.wait()
    total = project(x, y) + project(other, y)
    for place, o in places[6:]:
        for n, half in enumerate(halves):
            y_relay(n, half, o, place % 2 == 0)
    total += project(x, down) + project(x, up) + project(other, down) + project(other, up)

    drain(tt.at[pl.ds(0, PLANE - 1)], tr)
    lane = lax.broadcasted_iota(jnp.int32, (ROWS, 128), 1)
    prompt_row = lax.broadcasted_iota(jnp.int32, (ROWS, 128), 0)
    lane_task = (lane % NTASK).astype(F32)
    lane_row = lane // NTASK == prompt_row

    def select(p, carry):
        task = jnp.concatenate([tt[p], tt[p]], axis=0)
        hit = jnp.where(lane_row & (task == lane_task), 1.0, 0.0)
        sel[rows(p), :] = hit.astype(BF16)
        return carry

    lax.fori_loop(0, PLANE, select, 0)
    for n, half in enumerate(halves):
        drain(mix_t.at[half, across], qr.at[n])
        total += project(half, across)

    tb[z] = total.astype(BF16)
    mate = pair * 2 + 1 - lax.rem(z, 2)

    def u_send(to):
        push(tb.at[z], tb.at[z], us, ur.at[along(to - z, 8, 0)], at_z(to)).start()

    def u_wait(source):
        push(tb.at[source], tb.at[source], us, ur.at[along(z - source, 8, 0)], at_z(source)).wait_recv()

    for hop in HOPS:
        to = along(-hop, 4, pair)
        for one in (mate,) if hop == 0 else (2 * to, 2 * to + 1):
            u_send(one)

    mine = pl.ds(pl.multiple_of(c * COLS, COLS), COLS)
    missing = pl.ds(pl.multiple_of((1 - c) * COLS, COLS), COLS)

    def features(at):
        return pl.ds(pl.multiple_of(at * 512, 512), 512)

    def fetch(k):
        to = g_behind[k]
        push(w.at[mine, features(to)], wx.at[g, mine], hs, hr.at[k], at_g(to)).start()

    def hand_over(k):
        block = wx.at[g_ahead[k], mine]
        push(block, block, hs, hr.at[k], at_g(g_ahead[k])).wait_recv()
        push(block, block, ks, kr.at[k], {"dp_1": 1 - c}).start()

    for k in EARLY:
        fetch(k)

    own_rows = rows(d)
    pieces = [along(hop, 4, pair) for hop in HOPS]
    for j, i in enumerate(pieces):
        if j == 0:
            pre(6, 12)
        for one in (mate,) if HOPS[j] == 0 else (2 * i, 2 * i + 1):
            u_wait(one)
        for which in range(2):
            part = slice(which * COLS, (which + 1) * COLS)
            table = jnp.concatenate([tb[2 * i, part, :], tb[2 * i + 1, part, :]], axis=0)
            out[i, :, which] = dot(sel[...], table, NT).astype(BF16).reshape(PLANE, ROWS, DH)
        for k, dd in partners:
            d_to, g_to = d_ahead[dd], g_behind[k]
            push(
                out.at[i, d_to * 8 + g_to], pp.at[i, g, :, own_rows, :], ps, pr.at[j, k], device(d_to, g_to)
            ).start()
        for which in range(2):
            pp[i, g, which, own_rows, :] = out[i, me, which]
    pre(18, 14)
    for k in EARLY:
        hand_over(k)

    def head(i, g_here):
        h = g_here * 4 + i
        lanes = pl.ds(pl.multiple_of(h * DH, DH), DH)
        q, cot = qv[:, lanes], cv[:, lanes]
        scores = dot(pp[i, g_here, 0], q, NT) * SCALE
        grad = dot(pp[i, g_here, 1], cot, NT)
        self_top = stat[h, 0:1]
        top = jnp.maximum(jnp.max(scores, axis=0, keepdims=True), self_top)
        exponent = jnp.exp(scores - top)
        shrink = jnp.exp(self_top - top)
        inverse = 1.0 / (shrink * stat[h, 1:2] + jnp.sum(exponent, axis=0, keepdims=True))
        attention = exponent * inverse
        self_scale = shrink * inverse
        stat[h, 3:4] = self_scale
        rounded = attention.astype(BF16)
        pat[h] = rounded
        inner = self_scale * stat[h, 2:3] + jnp.sum(attention * grad, axis=0, keepdims=True)
        grad_scores = (attention * (grad - inner)).astype(BF16)
        gg[i, g_here, 0] = (dot(grad_scores, q) * SCALE).astype(BF16)
        gg[i, g_here, 1] = dot(rounded, cot).astype(BF16)

    def mid_step(j, i, ks, own_first):
        groups = [along(k, 8, g) for k in ks]
        for n, (k, g_here) in enumerate(zip(ks, groups)):
            if own_first and n == 0:
                drain(pp.at[i, g_here, :, pl.ds(0, PTOK - ROWS), :], pr.at[j, k])
            else:
                drain(pp.at[i, g_here], pr.at[j, k])
        for g_here in groups:
            head(i, g_here)
        for n, g_here in enumerate(groups):
            for dd in range(1 if own_first and n == 0 else 0, 4):
                d_to = d_ahead[dd]
                push(
                    gg.at[i, g_here, :, rows(d_to), :], rg.at[i, me], gs, gr.at[j], device(d_to, g_here)
                ).start()

    for j in MID:
        i = pieces[j]
        mid_step(j, i, list(range(MID_HEADS)), True)
        rg[i, me] = gg[i, g, :, own_rows, :]

        def later(n, carry, j=j, i=i):
            mid_step(j, i, [n * MID_HEADS + e for e in range(MID_HEADS)], False)
            return carry

        lax.fori_loop(1, 8 // MID_HEADS, later, 0)

    def post(first, count):
        def step(n, carry):
            for e in range(POST_HEADS):
                h = first + n * POST_HEADS + e
                lanes = pl.ds(pl.multiple_of(h * DH, DH), DH)
                self_part = (self_e[h] * stat[h, 3:4]).astype(BF16)
                prompt_values = pp[lax.rem(h, 4), lax.div(h, 4), 1]
                summed = dot(self_part, vv[:, lanes], TN) + dot(pat[h], prompt_values, TN)
                attended[:, lanes] = summed.astype(BF16)
            return carry

        lax.fori_loop(0, count // POST_HEADS, step, 0)

    for k in LATE:
        fetch(k)
    post(0, 8)

    for j in MID:
        i = pieces[j]
        drain(rg.at[i, pl.ds(0, PLANE - 1)], gr.at[j])
        for which in range(2):
            summed = dot(rg[i, :, which].reshape(PLANE * ROWS, DH), sel[...], TN).astype(BF16)
            part = slice(which * COLS, (which + 1) * COLS)
            gz[2 * i, part, :] = summed[:COLS]
            gz[2 * i + 1, part, :] = summed[COLS:]
        for to in (mate,) if HOPS[j] == 0 else (2 * i, 2 * i + 1):
            push(gz.at[to], rz.at[along(to - z, 8, 0)], bs, br, at_z(to)).start()
    for k in LATE:
        hand_over(k)
    post(8, 8)
    grad = gz[z].astype(F32)
    drain(rz.at[pl.ds(1, 7)], br)
    for o in range(1, 8):
        grad += rz[o].astype(F32)
    gt[g] = grad.astype(BF16)

    for k in reversed(NEAR):
        push(gt.at[g], gt.at[g], cs, cr.at[k], at_g(g_behind[k])).start()
    post(16, 10)
    terms = dot(w[:, features(g)], gt[g], TN)
    for k in NEAR:
        source = g_ahead[k]
        block = wx.at[source, missing]
        push(block, block, ks, kr.at[k], {"dp_1": 1 - c}).wait_recv()
        push(gt.at[source], gt.at[source], cs, cr.at[k], at_g(source)).wait_recv()
        terms += dot(wx[source], gt[source], TN)
    t2[...] = terms.astype(BF16).reshape(8, COLS, 128)
    for o in reversed(RING):
        to = along(o, 8, z)
        push(t2.at[to], rz2.at[o], es, er, at_z(to)).start()
    post(26, 6)
    mix = soft(logits[...])
    mixture_grad = t2[z].astype(F32)
    drain(rz2.at[pl.ds(1, 7)], er)
    for o in range(1, 8):
        mixture_grad += rz2[o].astype(F32)

    flipped = mixture_grad.T
    high = flipped.astype(BF16).astype(F32)
    middle = (flipped - high).astype(BF16).astype(F32)
    low = flipped - high - middle
    part = jnp.zeros((4 * NTASK, NSRC), F32)
    for r in range(ROWS):
        these = slice(r * NTASK, (r + 1) * NTASK)
        terms = jnp.concatenate([high[these], middle[these], low[these], jnp.zeros_like(low[these])], axis=0)
        part += dot(terms.astype(BF16), spv[r])
    part = part[:NTASK] + part[NTASK : 2 * NTASK] + part[2 * NTASK : 3 * NTASK]
    wslot[me] = part

    for k, dd in partners:
        push(wslot.at[me], wslot.at[me], ws, wr, device(d_ahead[dd], g_behind[k])).start()
    tile = jnp.concatenate([mix] * ROWS, axis=0)
    lane = lax.broadcasted_iota(jnp.int32, (COLS, 128), 1)
    for r in range(ROWS):
        chosen = jnp.where(lane // NTASK == r, mixture_grad, 0.0)
        source_grad[r] = jnp.dot(chosen, tile, precision=HIGH, preferred_element_type=F32)
    drain(wslot.at[pl.ds(0, PLANE - 1)], wr)
    wz[z] = jnp.sum(wslot[...], axis=0)
    for o in reversed(RING):
        push(wz.at[z], wz.at[z], vs, vr, at_z(along(o, 8, z))).start()
    drain(mix_t.at[0, y, z], xs)
    drain(mix_t.at[:, y, pl.ds(0, 7)], zs)
    drain(mix_t.at[:, pl.ds(0, 2)], ys)
    drain(mix_t.at[:, y], qs)
    drain(tt.at[pl.ds(0, PLANE - 1)], ts)
    drain(tb.at[pl.ds(0, 7)], us)
    drain(out.at[:, pl.ds(0, PLANE - 1)], ps)
    drain(rg.at[:, pl.ds(0, PLANE - 1)], gs)
    drain(gz.at[pl.ds(0, 7)], bs)
    drain(wx.at[pl.ds(0, 7), mine], hs)
    drain(wx.at[pl.ds(0, 7), mine], ks)
    drain(gt.at[pl.ds(0, 7)], cs)
    drain(t2.at[pl.ds(0, 7)], es)
    drain(wslot.at[pl.ds(0, PLANE - 1)], ws)
    drain(wz.at[pl.ds(0, 7)], vr)
    weight_grad = jnp.sum(wz[...], axis=0)
    logits_grad[...] = mix * (weight_grad - jnp.sum(mix * weight_grad, axis=1, keepdims=True))
    drain(wz.at[pl.ds(0, 7)], vs)


def finish_kernel(attended, source_grad, logits_grad, attended_out, source_out, logits_out, sems):
    given = ((attended, attended_out), (source_grad, source_out), (logits_grad, logits_out))
    copies = [pltpu.make_async_copy(one, to, sems.at[n]) for n, (one, to) in enumerate(given)]
    for one in copies:
        one.start()
    for one in copies:
        one.wait()


def finish(*given):
    vmem = pl.BlockSpec(memory_space=pltpu.VMEM)
    any_space = pl.BlockSpec(memory_space=pl.ANY)
    return pl.pallas_call(
        finish_kernel,
        out_shape=tuple(jax.ShapeDtypeStruct(one.shape, one.dtype) for one in given),
        in_specs=[vmem] * 3,
        out_specs=(any_space,) * 3,
        scratch_shapes=[pltpu.SemaphoreType.DMA((3,))],
        name="prompt_finish",
    )(*(pltpu.with_memory_space_constraint(one, pltpu.VMEM) for one in given))


def on_device(source_prompts, task_logits, task_ids, key_weight, value_weight, queries, keys, values, cotangent):
    any_space = pl.BlockSpec(memory_space=pl.ANY)
    vmem = pl.BlockSpec(memory_space=pltpu.VMEM)
    dma = pltpu.SemaphoreType.DMA
    attended, source_grad, logits_grad = pl.pallas_call(
        kernel,
        out_shape=(
            pltpu.VMEM((SEQ, D), BF16),
            pltpu.VMEM((ROWS, COLS, NSRC), F32),
            pltpu.VMEM((NTASK, NSRC), F32),
        ),
        in_specs=[pl.BlockSpec(memory_space=pltpu.SMEM), vmem] + [any_space] * 7,
        out_specs=(vmem, vmem, vmem),
        scratch_shapes=[
            pltpu.VMEM((ROWS, COLS, NSRC), BF16),
            pltpu.VMEM((2 * COLS, D), BF16),
            pltpu.VMEM((8, 2 * COLS, 512), BF16),
            *[pltpu.VMEM((SEQ, D), BF16)] * 4,
            pltpu.VMEM((2, 4, 8, COLS, 128), BF16),
            pltpu.VMEM((8, 128, 128), BF16),
            pltpu.VMEM((PLANE, 8, 128), F32),
            pltpu.VMEM((PLANE * ROWS, 128), BF16),
            pltpu.VMEM((4, PLANE, 2, ROWS, DH), BF16),
            pltpu.VMEM((4, 8, 2, PTOK, DH), BF16),
            pltpu.VMEM((HEADS, 8, SEQ), F32),
            pltpu.VMEM((HEADS, SEQ, SEQ), F32),
            pltpu.VMEM((HEADS, PTOK, SEQ), BF16),
            pltpu.VMEM((4, 8, 2, PTOK, DH), BF16),
            pltpu.VMEM((4, PLANE, 2, ROWS, DH), BF16),
            pltpu.VMEM((8, 128, 128), BF16),
            pltpu.VMEM((8, 128, 128), BF16),
            pltpu.VMEM((8, 128, 128), BF16),
            pltpu.VMEM((8, COLS, 128), BF16),
            pltpu.VMEM((8, COLS, 128), BF16),
            pltpu.VMEM((PLANE, NTASK, NSRC), F32),
            pltpu.VMEM((8, NTASK, NSRC), F32),
            dma((7,)), dma, dma((2, 8)), dma, dma, dma, dma((2, 2, 8)), dma, dma((2,)), dma, dma((8,)),
            dma, dma, dma, dma((4, 8)), dma, dma((4,)), dma, dma((8,)), dma, dma((8,)),
            dma, dma, dma, dma((8,)), dma, dma,
            dma, dma, dma, dma,
        ],
        compiler_params=pltpu.CompilerParams(collective_id=0, has_side_effects=True),
        name="prompt_step",
    )(
        task_ids, task_logits, source_prompts.transpose(1, 2, 0), key_weight.T, value_weight.T,
        queries[0], keys[0], values[0], cotangent[0],
    )
    attended, source_grad, logits_grad = finish(attended, source_grad, logits_grad)
    return attended[None], source_grad.transpose(2, 0, 1), logits_grad


def solution(mesh):
    torus = Mesh(mesh.devices.reshape(2, 2, 2, 4, 8), AXES)
    return jax.shard_map(
        on_device,
        mesh=torus,
        in_specs=(
            P(None, None, MP),
            P(),
            P(DP),
            P(None, MP),
            P(None, MP),
            P(AXES, None, None),
            P(AXES, None, None),
            P(AXES, None, None),
            P(AXES, None, None),
        ),
        out_specs=(P(AXES, None, None), P(None, DP, MP), P()),
        check_vma=False,
    )
```
